32 devices in a mesh: grp: 2 (over x), tile: 16 (over z, y, core).
Axes of the slice: x: 2, y: 2, z: 4, core: 2. Of those that a mesh axis runs over, the one named last changes fastest.
Arguments:
- habitat: int32 [32, 4, 512], P(('grp', 'tile')), parts along dimension 0, may hold values from 0 to 15
- table: float32 [16], replicated, may hold values from 0.25 to 2
- source_cell: int32 [512], P('grp'), parts along dimension 0, may hold values from 0 to 32767
- ground_cell: int32 [512], P('grp'), parts along dimension 0, may hold values from 0 to 32767
- start_potential: float32 [32, 4, 512, 256], P(('grp', 'tile')), parts along dimension 0, may hold values from -30 to 30
Outputs:
- potentials: float32 [32, 4, 512, 256], P(('grp', 'tile')), parts along dimension 0
- residual: float32 [32, 4, 512, 256], P(('grp', 'tile')), parts along dimension 0
- resistance: float32 [512], P('grp'), parts along dimension 0
The draws below stay inside these ranges and needn't reach their ends.
There are 2 independent parts, one for each index of `grp`. The reference program is written for one: setup_inputs(seed, part) draws one part's arguments, and reference() takes and returns one part's arrays. A program takes and returns all parts, laid end to end along the dimension named above; an argument that names none is the same for every part. Nothing has to cross between parts.
Inputs may be any that keep to these rules, and one draw needn't show every extreme that they name: `source_cell`: an index row * 1024 + column of the raster. `ground_cell`: an index row * 1024 + column of the raster.
All inputs are finite; a program needn't handle non-finite values.
Results may differ from the reference program's by a relative error of at most 0.00018.
Values sent between devices are 32-bit elements; how exact they have to be, the bound alone decides.
A program may use at most 128 MiB of HBM per device.

```python
import math
import jax
import jax.numpy as jnp

CX = 4
CY = 512
R = 256
CLASSES = 16
ITERS = 2
BLOCKS = 16
NX = 32
NY = 1024


def draw_start_potential(key, part):
    base_key = jax.random.fold_in(jax.random.fold_in(key, 17), 0)
    block_rows = jnp.arange(BLOCKS) // 2
    raster_rows = block_rows[:, None] * CX + jnp.arange(CX)[None, :]
    ramp = jnp.exp(1.1513 * raster_rows.astype(jnp.float32) / max(NX - 1, 1))
    field = jax.random.normal(base_key, (BLOCKS, CX, CY, R), jnp.float32)
    return field * ramp[:, :, None, None]


def set_ends(result, rng, low, largest):
    longest = result.shape.index(max(result.shape))
    spots = []
    for shift in (0, 1):
        where = [jax.random.randint(jax.random.fold_in(rng, axis), (), 0, length) for axis, length in enumerate(result.shape)]
        where[longest] = (where[longest] + shift) % result.shape[longest]
        spots.append(tuple(where))
    return result.at[spots[0]].set(low).at[spots[1]].set(largest)


def setup_inputs(seed: int = 0, part: int = 0) -> dict:
    keys = jax.random.split(jax.random.key(seed), 6)
    part_splits = jax.random.split(jax.random.fold_in(keys[5], part), 6)
    habitat = set_ends(jax.random.randint(part_splits[0], (BLOCKS, CX, CY), 0, CLASSES), jax.random.fold_in(part_splits[0], 1), 0, CLASSES - 1).astype(jnp.int32)
    table = jnp.clip(jnp.exp(jax.random.uniform(keys[1], (CLASSES,), jnp.float32, math.log(0.25), math.log(2.0))), 0.25, 2.0)
    source_cell = set_ends(jax.random.randint(part_splits[2], (R,), 0, NX * NY), jax.random.fold_in(part_splits[2], 1), 0, (NX * NY) - 1).astype(jnp.int32)
    ground_cell = set_ends(jax.random.randint(part_splits[3], (R,), 0, NX * NY), jax.random.fold_in(part_splits[3], 1), 0, (NX * NY) - 1).astype(jnp.int32)
    start_potential = draw_start_potential(jax.random.fold_in(jax.random.fold_in(keys[5], part), 71), part)
    return dict(habitat=habitat, table=table, source_cell=source_cell, ground_cell=ground_cell, start_potential=start_potential)


def to_raster(blocks):
    block_count, rows_here, cols_here = blocks.shape[0], blocks.shape[1], blocks.shape[2]
    trailing = blocks.shape[3:]
    blocks_grid = blocks.reshape((block_count // 2, 2, rows_here, cols_here) + trailing)
    blocks_grid = jnp.swapaxes(blocks_grid, 1, 2)
    return blocks_grid.reshape((block_count // 2 * rows_here, 2 * cols_here) + trailing)


def to_blocks(raster, rows_here, cols_here):
    trailing = raster.shape[2:]
    blocks_grid = raster.reshape((raster.shape[0] // rows_here, rows_here, 2, cols_here) + trailing)
    blocks_grid = jnp.swapaxes(blocks_grid, 1, 2)
    return blocks_grid.reshape((raster.shape[0] // rows_here * 2, rows_here, cols_here) + trailing)


def reference(habitat, table, source_cell, ground_cell, start_potential):
    classes = to_raster(habitat)
    conduct = table[classes]
    row_count, col_count = classes.shape[0], classes.shape[1]
    padded = jnp.pad(conduct, 1)
    row_index = jnp.arange(row_count)[:, None]
    col_index = jnp.arange(col_count)[None, :]
    north_w = jnp.where(row_index > 0, 0.5 * (conduct + padded[:-2, 1:-1]), 0.0)
    south_w = jnp.where(row_index < row_count - 1, 0.5 * (conduct + padded[2:, 1:-1]), 0.0)
    west_w = jnp.where(col_index > 0, 0.5 * (conduct + padded[1:-1, :-2]), 0.0)
    east_w = jnp.where(col_index < col_count - 1, 0.5 * (conduct + padded[1:-1, 2:]), 0.0)
    cell_ids = (row_index * col_count + col_index).astype(jnp.int32)
    ground_mask = (cell_ids[:, :, None] == ground_cell[None, None, :]).astype(jnp.float32)
    diagonal = (north_w + south_w + west_w + east_w)[:, :, None] + ground_mask
    source_field = (cell_ids[:, :, None] == source_cell[None, None, :]).astype(jnp.float32)

    def operate(field):
        pad_field = jnp.pad(field, ((1, 1), (1, 1), (0, 0)))
        applied = diagonal * field - north_w[:, :, None] * pad_field[:-2, 1:-1]
        applied = applied - south_w[:, :, None] * pad_field[2:, 1:-1]
        applied = applied - west_w[:, :, None] * pad_field[1:-1, :-2]
        return applied - east_w[:, :, None] * pad_field[1:-1, 2:]

    potentials = to_raster(start_potential)
    residual = source_field - operate(potentials)
    direction = residual
    norm_now = jnp.sum(residual * residual, axis=(0, 1))
    for iteration in range(ITERS):
        applied = operate(direction)
        step_size = norm_now / jnp.sum(direction * applied, axis=(0, 1))
        potentials = potentials + step_size * direction
        residual = residual - step_size * applied
        if iteration + 1 < ITERS:
            norm_next = jnp.sum(residual * residual, axis=(0, 1))
            direction = residual + (norm_next / norm_now) * direction
            norm_now = norm_next
    flattened = potentials.reshape((row_count * col_count, potentials.shape[2]))
    columns = jnp.arange(potentials.shape[2], dtype=jnp.int32)
    resistance = flattened[source_cell, columns] - flattened[ground_cell, columns]
    rows_here, cols_here = habitat.shape[1], habitat.shape[2]
    return to_blocks(potentials, rows_here, cols_here), to_blocks(residual, rows_here, cols_here), resistance
```

```python
import functools

import jax
import jax.numpy as jnp
from jax import lax
from jax.experimental import pallas as pl
from jax.experimental.pallas import tpu as pltpu
from jax.sharding import PartitionSpec as P

LANES = 128
TILE = 8
PAD = 2 * TILE
MESH = pl.DeviceIdType.MESH


def cuts(total, weights):
    bounds, seen = [0], 0
    for weight in weights:
        seen += weight
        bounds.append(total * seen // sum(weights))
    return bounds


def kernel(n, rows, cols, rounds, shared_weights, own_weights,
           table_hbm, habitat_hbm, source_hbm, ground_hbm, start_ref,
           pot_ref, res_ref, field_ref, coef_ref, drop_ref,
           X, R, W, U, V, H, D, C, T, TV, TH, S,
           table_ref, habitat_ref, source_ref, ground_ref, small_sem, load_sem,
           cond_recv, side_recv, edge_recv, cross_recv, shared_recv, relay_recv, near_recv, far_recv,
           sum_recv, cond_send, side_send, cross_send, near_send, far_send, relay_send, sum_send, hello):
    halves = X.shape[0]
    width = cols + 2 * PAD
    me = lax.axis_index("tile")
    chips = n // 2
    chip = me // 2
    core = me % 2
    odd = chip % 2
    side = me + 1 - 2 * core
    partner = me + 2 - 4 * odd
    diagonal = me - 2 + 4 * odd
    relay_to = me + 4 - 8 * odd
    relay_from = me - 4 + 8 * odd
    has_above = chip > 0
    has_below = chip < chips - 1
    has_diagonal = jnp.where(odd == 0, chip > 0, chip < chips - 1)
    can_relay = jnp.where(odd == 0, chip + 2 < chips, chip >= 2)
    gets_relay = jnp.where(odd == 0, chip >= 2, chip + 2 < chips)
    own = pl.ds(PAD, cols)
    body = cols // TILE - 1
    shared_at = cuts(body, shared_weights)
    own_at = [cuts(body, weights) for weights in own_weights]

    def remote(src, dst, send, recv, target):
        return pltpu.make_async_remote_copy(
            src_ref=src, dst_ref=dst, send_sem=send, recv_sem=recv,
            device_id={"tile": target}, device_id_type=MESH)

    def arrived(place, recv):
        remote(place, place, near_send.at[0], recv, partner).wait_recv()

    def drained(place, send):
        remote(place, place, send, sum_recv.at[0], partner).wait_send()

    def signal(sem, target):
        pl.semaphore_signal(sem, inc=1, device_id={"tile": target}, device_id_type=MESH)

    def load(h):
        return pltpu.make_async_copy(
            start_ref.at[0, :, :, pl.ds(h * LANES, LANES)], X.at[h, pl.ds(rows, rows), own, :],
            load_sem.at[h])

    smalls = [
        pltpu.make_async_copy(src, dst, small_sem.at[k])
        for k, (src, dst) in enumerate((
            (table_hbm, table_ref), (habitat_hbm, habitat_ref),
            (source_hbm, source_ref), (ground_hbm, ground_ref)))
    ]

    barrier = pltpu.get_barrier_semaphore()
    signal(barrier, side)

    @pl.when(has_above)
    def _():
        signal(barrier, me - 2)
        signal(barrier, side - 2)

    @pl.when(has_below)
    def _():
        signal(barrier, me + 2)
        signal(barrier, side + 2)

    @pl.when(gets_relay)
    def _():
        signal(barrier, relay_from)

    for h in range(halves):
        load(h).start()
    for copy in smalls:
        copy.start()

    inner = pl.multiple_of(PAD + (1 - core) * (cols - TILE), TILE)
    outer = pl.multiple_of((1 - core) * TILE + core * (PAD + cols), TILE)
    halo = pl.multiple_of(core * TILE + (1 - core) * (PAD + cols), TILE)
    inner_at, outer_at, halo_at = pl.ds(inner, TILE), pl.ds(outer, TILE), pl.ds(halo, TILE)

    def span(bounds, j):
        start = pl.multiple_of(PAD + core * TILE + bounds[j] * TILE, TILE)
        return pl.ds(start, (bounds[j + 1] - bounds[j]) * TILE)

    def side_copy(h):
        place = pl.ds(rows, rows)
        return remote(X.at[h, place, inner_at, :], X.at[h, place, outer_at, :],
                      side_send.at[0], side_recv.at[h], side)

    def side_wait(h):
        arrived(X.at[h, pl.ds(rows, rows), halo_at, :], side_recv.at[h])

    def edge_near(h):
        return remote(X.at[h, pl.ds(rows + 1 - odd, rows - 1), inner_at, :],
                      X.at[h, pl.ds(odd * 2 * rows + 1 - odd, rows - 1), inner_at, :],
                      near_send.at[0], edge_recv.at[h, 0], partner)

    def edge_far(h):
        return remote(X.at[h, pl.ds(rows + odd, rows - 1), inner_at, :],
                      X.at[h, pl.ds((1 - odd) * 2 * rows + odd, rows - 1), inner_at, :],
                      far_send.at[0], edge_recv.at[h, 1], diagonal)

    near_rows = pl.ds((1 - odd) * 2 * rows + odd, rows - 1)
    far_rows = pl.ds(odd * 2 * rows + 1 - odd, rows - 1)

    def cross(h, k):
        place = (near_rows, far_rows)[k]
        return remote(X.at[h, place, inner_at, :], X.at[h, place, outer_at, :],
                      cross_send.at[k], cross_recv.at[h, k], side)

    def cross_wait(h, k):
        arrived(X.at[h, (near_rows, far_rows)[k], halo_at, :], cross_recv.at[h, k])

    def shared_copy(h, j):
        at = span(shared_at, j)
        return remote(X.at[h, pl.ds(rows + 1, rows - 2), at, :],
                      X.at[h, pl.ds(odd * 2 * rows + 1, rows - 2), at, :],
                      near_send.at[0], shared_recv.at[h, j], partner)

    def relay_copy(h, j):
        at = span(shared_at, j)
        return remote(X.at[h, pl.ds((1 - odd) * 2 * rows + 1, rows - 2), at, :],
                      X.at[h, pl.ds(odd * 2 * rows + 1, rows - 2), at, :],
                      relay_send.at[0], relay_recv.at[h, j], relay_to)

    def near_copy(h, k):
        at = span(own_at[h], k)
        row = (1 - odd) * (rows - 1)
        return remote(X.at[h, rows + row, at, :], X.at[h, odd * 2 * rows + row, at, :],
                      near_send.at[0], near_recv.at[h, k], partner)

    def far_copy(h, k):
        at = span(own_at[h], k)
        row = odd * (rows - 1)
        return remote(X.at[h, rows + row, at, :], X.at[h, (1 - odd) * 2 * rows + row, at, :],
                      far_send.at[0], far_recv.at[h, k], diagonal)

    pl.semaphore_wait(
        barrier,
        1 + 2 * has_above.astype(jnp.int32) + 2 * has_below.astype(jnp.int32) + can_relay.astype(jnp.int32))

    for h in range(halves):
        load(h).wait()
        side_copy(h).start()
        edge_near(h).start()

        @pl.when(has_diagonal)
        def _():
            edge_far(h).start()

    for h in range(halves):
        for j in range(len(shared_weights)):
            shared_copy(h, j).start()
        for k in range(len(own_weights[h])):
            @pl.when(has_diagonal)
            def _():
                far_copy(h, k).start()
            near_copy(h, k).start()

    for copy in smalls:
        copy.wait()
    cells = habitat_ref[0]
    cond = jnp.zeros(cells.shape, jnp.float32)
    for level in range(table_ref.shape[0]):
        cond = jnp.where(cells == level, table_ref[level], cond)
    C[5, 0:rows, :] = cond
    C[5, rows:2 * rows, :] = cond

    def cond_copy(target, slot, kind):
        return remote(C.at[5], C.at[slot], cond_send.at[kind], cond_recv.at[slot], target)

    cond_copy(side, 2, 0).start()

    @pl.when(has_above)
    def _():
        cond_copy(me - 2, 1, 1).start()
        cond_copy(side - 2, 4, 1).start()

    @pl.when(has_below)
    def _():
        cond_copy(me + 2, 0, 2).start()
        cond_copy(side + 2, 3, 2).start()

    def zero(ref, h, c):
        ref[h, :, c:c + TILE, :] = jnp.zeros((ref.shape[1], TILE, LANES), jnp.float32)

    for h in range(halves):
        for c in (0, width - TILE):
            zero(X, h, c)
            zero(R, h, c)
            zero(W, h, c)

        @pl.when(core == 0)
        def _():
            zero(X, h, TILE)

        @pl.when(core == 1)
        def _():
            zero(X, h, width - PAD)

        @pl.when(jnp.logical_not(has_above))
        def _():
            X[h, 0:rows] = jnp.zeros((rows, width, LANES), jnp.float32)

        @pl.when(jnp.logical_not(has_below))
        def _():
            X[h, 2 * rows:3 * rows] = jnp.zeros((rows, width, LANES), jnp.float32)

    for h in range(halves):
        arrived(X.at[h, near_rows, inner_at, :], edge_recv.at[h, 0])
        cross(h, 0).start()

    @pl.when(has_diagonal)
    def _():
        for h in range(halves):
            arrived(X.at[h, far_rows, inner_at, :], edge_recv.at[h, 1])
            cross(h, 1).start()

    arrived(C.at[2], cond_recv.at[2])

    @pl.when(has_above)
    def _():
        arrived(C.at[0], cond_recv.at[0])
        arrived(C.at[3], cond_recv.at[3])

    @pl.when(has_below)
    def _():
        arrived(C.at[1], cond_recv.at[1])
        arrived(C.at[4], cond_recv.at[4])

    @pl.when(jnp.logical_not(has_above))
    def _():
        for slot in (0, 3):
            C[slot] = jnp.zeros(C.shape[1:], jnp.float32)

    @pl.when(jnp.logical_not(has_below))
    def _():
        for slot in (1, 4):
            C[slot] = jnp.zeros(C.shape[1:], jnp.float32)

    def greet(r):
        d = 2 << r

        @pl.when(me >= d)
        def _():
            signal(hello.at[r], me - d)

        @pl.when(me + d < n)
        def _():
            signal(hello.at[r], me + d)

    def greeted(r):
        d = 2 << r
        pl.semaphore_wait(hello.at[r], (me >= d).astype(jnp.int32) + (me + d < n).astype(jnp.int32))

    greet(0)

    first = lax.broadcasted_iota(jnp.int32, (2 * rows, LANES), 0) < rows

    def turned(above, here, below, j):
        lanes = slice(j * LANES, (j + 1) * LANES)
        top = jnp.where(first, C[above, :, lanes], C[here, :, lanes])
        blank = jnp.zeros((LANES - 4 * rows, LANES), jnp.float32)
        return jnp.transpose(jnp.concatenate([top, C[below, :, lanes], blank], 0))

    for j in range(cols // LANES):
        T[PAD + j * LANES:PAD + (j + 1) * LANES, :] = turned(0, 5, 1, j)
    for c in (0, TILE, width - PAD, width - TILE):
        T[c:c + TILE, :] = jnp.zeros((TILE, LANES), jnp.float32)

    @pl.when(core == 0)
    def _():
        T[width - PAD:width - TILE, :] = turned(3, 2, 4, 0)[0:TILE]

    @pl.when(core == 1)
    def _():
        T[TILE:PAD, :] = turned(3, 2, 4, cols // LANES - 1)[LANES - TILE:]

    def global_col(c):
        return core * cols - PAD + c + lax.broadcasted_iota(jnp.int32, (TILE, LANES), 0)

    global_row = chip * rows - rows + lax.broadcasted_iota(jnp.int32, (TILE, LANES), 1)
    total_rows, total_cols = chips * rows, 2 * cols

    def edges(t, _):
        c = pl.multiple_of(t * TILE, TILE)
        here = T[pl.ds(c, TILE), :]
        east = T[pl.ds(c + 1, TILE), :]
        south = pltpu.roll(here, LANES - 1, 1)
        gc = global_col(c)
        in_row = (global_row >= 0) & (global_row < total_rows - 1)
        TV[pl.ds(c, TILE), :] = jnp.where(in_row, 0.5 * (here + south), 0.0)
        in_col = (gc >= 0) & (gc < total_cols - 1)
        TH[pl.ds(c, TILE), :] = jnp.where(in_col, 0.5 * (here + east), 0.0)
        return 0

    TH[0:TILE, :] = jnp.zeros((TILE, LANES), jnp.float32)
    H[:, 0:TILE, :] = jnp.zeros((H.shape[0], TILE, LANES), jnp.float32)
    lax.fori_loop(1, width // TILE - 1, edges, 0, unroll=2)

    def spread(t, _):
        c = pl.multiple_of(t * TILE, TILE)
        at = pl.ds(c, TILE)
        v = TV[at, :]
        east = TH[at, :]
        west = TH[pl.ds(c - 1, TILE), :]
        diag = v + pltpu.roll(v, 1, 1) + east + west
        shape = (TILE, LANES)
        for k in range(2 * rows + 1):
            V[k, at, :] = jnp.broadcast_to(v[:, k + 1:k + 2], shape)
        for k in range(2 * rows):
            H[k, at, :] = jnp.broadcast_to(east[:, k + 2:k + 3], shape)
            D[k, at, :] = jnp.broadcast_to(diag[:, k + 2:k + 3], shape)
        return 0

    tiles = width // TILE

    def relay(h, j):
        arrived(X.at[h, pl.ds((1 - odd) * 2 * rows + 1, rows - 2), span(shared_at, j), :],
                shared_recv.at[h, j])

        @pl.when(can_relay)
        def _():
            relay_copy(h, j).start()

    parts = len(shared_weights)
    splits = cuts(tiles - 2, [1] * parts)
    for j in range(parts):
        lax.fori_loop(1 + splits[j], 1 + splits[j + 1], spread, 0)
        relay(0, j)
        if j < rounds:
            greeted(j)
            if j + 1 < rounds:
                greet(j + 1)
    for r in range(parts, rounds):
        greeted(r)
        if r + 1 < rounds:
            greet(r + 1)

    def ends(h, lag, first, end):
        return [first] + [PAD // TILE + core + bound - lag for bound in own_at[h][1:-1]] + [end]

    def shape_of(cells, h, top):
        base = (chip * rows + top) * total_cols + core * cols - PAD
        return jnp.broadcast_to(cells[h:h + 1, :] - base, (TILE, LANES))

    def applied(ref, h, skip, count, c, low, grounds):
        at = pl.ds(c, TILE)
        west = pl.ds(c - 1, TILE)
        east = pl.ds(c + 1, TILE)
        column = c + lax.broadcasted_iota(jnp.int32, (TILE, LANES), 0)
        mid = ref[h, skip + 1, at, :]
        flow = V[low, at, :] * ref[h, skip, at, :]
        for k in range(count):
            after = ref[h, skip + k + 2, at, :]
            v = V[low + k + 1, at, :]
            grounded = column == grounds[k]
            diag = D[low + k, at, :]
            out = jnp.where(grounded, diag + 1.0, diag) * mid - flow
            out = out - v * after
            out = out - H[low + k, west, :] * ref[h, skip + 1 + k, west, :]
            out = out - H[low + k, at, :] * ref[h, skip + 1 + k, east, :]
            yield k, out, mid, grounded, column
            flow = v * mid
            mid = after

    def zeros():
        return tuple(jnp.zeros((TILE, LANES), jnp.float32) for _ in range(7))

    def compute(h, j, acc):
        def named(cells, top, count):
            return [shape_of(cells, h, top + k) for k in range(count)]

        count_r, count_w = 2 * rows, 2 * rows - 2
        src_r, gnd_r = named(source_ref, -2, count_r), named(ground_ref, -2, count_r)
        gnd_w = named(ground_ref, -1, count_w)
        src_u, gnd_u = named(source_ref, 0, rows), named(ground_ref, 0, rows)

        def pass_r(t, _):
            c = pl.multiple_of(t * TILE, TILE)
            for k, a, _mid, _g, column in applied(X, h, 1, count_r, c, 0, gnd_r):
                R[h, k, pl.ds(c, TILE), :] = jnp.where(column == src_r[k], 1.0 - a, -a)
            return 0

        def pass_w(t, _):
            c = pl.multiple_of(t * TILE, TILE)
            for k, a, _mid, _g, _column in applied(R, h, 0, count_w, c, 1, gnd_w):
                W[h, k, pl.ds(c, TILE), :] = a
            return 0

        def pass_u(t, acc):
            c = pl.multiple_of(t * TILE, TILE)
            at = pl.ds(c, TILE)
            to = pl.ds(c - PAD, TILE)
            for k, u, w, grounded, column in applied(W, h, 0, rows, c, 2, gnd_u):
                r = R[h, 2 + k, at, :]
                x = X[h, rows + k, at, :]
                if h < halves - 1:
                    U[h, k, to, :] = u
                else:
                    for place, value in enumerate((x, r, w, u)):
                        field_ref[place, k, to, :] = value
                sign = jnp.where(column == src_u[k], 1.0, 0.0) - jnp.where(grounded, 1.0, 0.0)
                terms = (r * r, r * w, w * w, w * u, sign * x, sign * r, sign * w)
                acc = tuple(s + term for s, term in zip(acc, terms))
            return acc

        r_ends, w_ends, u_ends = (
            ends(h, lag, 1 + (lag == 3), tiles - 1 - (lag == 3)) for lag in (1, 2, 3))
        lax.fori_loop(r_ends[j], r_ends[j + 1], pass_r, 0)
        lax.fori_loop(w_ends[j], w_ends[j + 1], pass_w, 0)
        return lax.fori_loop(u_ends[j], u_ends[j + 1], pass_u, acc)

    def sum_copy(h, d):
        return remote(S.at[h, me], S.at[h, me], sum_send.at[0], sum_recv.at[h], (me + d) % n)

    def send_sums(h, acc):
        sums = [jnp.sum(s, axis=0, keepdims=True) for s in acc]
        S[h, me] = jnp.concatenate(sums + [jnp.zeros((1, LANES), jnp.float32)], 0)
        lax.fori_loop(1, n, lambda d, _: (sum_copy(h, d).start(), 0)[1], 0)

    def totals(h):
        arrived(S.at[h, pl.ds(0, n - 1)], sum_recv.at[h])
        total = S[h, 0]
        for k in range(1, n):
            total = total + S[h, k]
        m0, m1, m2, m3, ex, er, ew = (total[k:k + 1] for k in range(7))
        a0 = m0 / m1
        next_norm = a0 * (a0 * m2 - m1)
        ratio = next_norm / m0
        curve = m1 - a0 * (2.0 * m2 - a0 * m3)
        a1 = next_norm / (curve - ratio * next_norm / a0)
        p = a0 + a1 * (1.0 + ratio)
        q = a1 * a0
        drop_ref[h:h + 1, :] = ex + p * er - q * ew
        return p, q

    def finish(h):
        p, q = totals(h)
        p1 = jnp.broadcast_to(p, (TILE, LANES))
        q1 = jnp.broadcast_to(q, (TILE, LANES))

        def last(t, _):
            c = pl.multiple_of(t * TILE, TILE)
            at = pl.ds(c + PAD, TILE)
            to = pl.ds(c, TILE)
            for k in range(rows):
                r = R[h, 2 + k, at, :]
                w = W[h, 1 + k, at, :]
                pot_ref[h, k, to, :] = X[h, rows + k, at, :] + p1 * r - q1 * w
                res_ref[h, k, to, :] = r - p1 * w + q1 * U[h, k, to, :]
            return 0

        lax.fori_loop(0, cols // TILE, last, 0)

    for h in range(halves):
        side_wait(h)
        cross_wait(h, 0)

        @pl.when(has_diagonal)
        def _():
            cross_wait(h, 1)

        acc = zeros()
        relayed = 0
        for k in range(len(own_weights[h])):
            while relayed < parts and shared_at[relayed] < own_at[h][k + 1]:
                @pl.when(gets_relay)
                def _():
                    arrived(X.at[h, pl.ds(odd * 2 * rows + 1, rows - 2), span(shared_at, relayed), :],
                            relay_recv.at[h, relayed])
                relayed += 1

            @pl.when(has_diagonal)
            def _():
                arrived(X.at[h, odd * 2 * rows + (1 - odd) * (rows - 1), span(own_at[h], k), :],
                        far_recv.at[h, k])
            arrived(X.at[h, (1 - odd) * 2 * rows + odd * (rows - 1), span(own_at[h], k), :],
                    near_recv.at[h, k])
            acc = compute(h, k, acc)
        send_sums(h, acc)
        if h < halves - 1:
            for j in range(parts):
                relay(h + 1, j)
                if j == parts // 2 - 1:
                    finish(h)

    p, q = totals(halves - 1)
    coef_ref[...] = jnp.concatenate([p, q, jnp.zeros((TILE - 2, LANES), jnp.float32)], 0)

    drained(C.at[0], cond_send.at[0])

    @pl.when(has_above)
    def _():
        drained(C.at[pl.ds(0, 2)], cond_send.at[1])

    @pl.when(has_below)
    def _():
        drained(C.at[pl.ds(0, 2)], cond_send.at[2])

    drained(X.at[:, pl.ds(0, rows), pl.ds(0, TILE), :], side_send.at[0])
    drained(X.at[:, pl.ds(0, rows - 1), pl.ds(0, TILE), :], cross_send.at[0])
    drained(X.at[:, pl.ds(0, rows - 1), pl.ds(0, cols), :], near_send.at[0])

    @pl.when(has_diagonal)
    def _():
        drained(X.at[:, pl.ds(0, rows - 1), pl.ds(0, TILE), :], cross_send.at[1])
        drained(X.at[:, pl.ds(0, 1), pl.ds(0, cols + (rows - 2) * TILE), :], far_send.at[0])

    @pl.when(can_relay)
    def _():
        drained(X.at[:, pl.ds(0, rows - 2), pl.ds(0, cols - TILE), :], relay_send.at[0])

    drained(S.at[:, pl.ds(0, n - 1)], sum_send.at[0])


def closing(pot_ref, res_ref, field_ref, coef_ref, drop_ref, pot_out, res_out, drop_out,
            P1, Q1, sem):
    rows, cols = field_ref.shape[1], field_ref.shape[2]
    before = pot_ref.shape[0]

    def put(ref, out, h, c, count, k):
        return pltpu.make_async_copy(
            ref.at[:, pl.ds(c, count), :],
            out.at[0, :, pl.ds(c, count), pl.ds(h * LANES, LANES)], sem.at[k])

    for h in range(before):
        put(pot_ref.at[h], pot_out, h, 0, cols, 0).start()
        put(res_ref.at[h], res_out, h, 0, cols, 1).start()
    drop = pltpu.make_async_copy(drop_ref, drop_out, sem.at[2])
    drop.start()

    p1 = jnp.broadcast_to(coef_ref[0:1, :], (TILE, LANES))
    q1 = jnp.broadcast_to(coef_ref[1:2, :], (TILE, LANES))
    pieces = 4
    step = cols // pieces

    def last(t, _):
        c = pl.multiple_of(t * TILE, TILE)
        at = pl.ds(c, TILE)
        for k in range(rows):
            x, r, w, u = (field_ref[place, k, at, :] for place in range(4))
            P1[k, at, :] = x + p1 * r - q1 * w
            Q1[k, at, :] = r - p1 * w + q1 * u
        return 0

    for piece in range(pieces):
        lax.fori_loop(piece * step // TILE, (piece + 1) * step // TILE, last, 0, unroll=2)
        put(P1, pot_out, before, piece * step, step, 0).start()
        put(Q1, res_out, before, piece * step, step, 1).start()

    for k, out in enumerate((pot_out, res_out)):
        pltpu.make_async_copy(out, out, sem.at[k]).wait()
    drop.wait()


def solution(mesh):
    n = mesh.shape["tile"]
    rounds = max(1, (n // 2 - 1).bit_length())

    def shards(habitat, table, source_cell, ground_cell, start_potential):
        _, rows, cols, rhs = start_potential.shape
        halves = rhs // LANES
        width = cols + 2 * PAD
        f32 = jnp.float32
        dma = pltpu.SemaphoreType.DMA
        field = jax.ShapeDtypeStruct(start_potential.shape, f32)
        part = jax.ShapeDtypeStruct((halves - 1, rows, cols, LANES), f32)
        drops = jax.ShapeDtypeStruct((halves, LANES), f32)
        vmem = pl.BlockSpec(memory_space=pltpu.VMEM)
        hbm = pl.BlockSpec(memory_space=pltpu.HBM)
        shared_weights = (16, 16, 16, 15)
        own_weights = ((16, 16, 16, 15),) * (halves - 1) + ((9, 9, 9, 9, 9, 8, 6, 4),)
        parts, most = len(shared_weights), max(map(len, own_weights))
        stages = pl.pallas_call(
            functools.partial(kernel, n, rows, cols, rounds, shared_weights, own_weights),
            out_shape=(part, part, jax.ShapeDtypeStruct((4, rows, cols, LANES), f32),
                       jax.ShapeDtypeStruct((TILE, LANES), f32), drops),
            in_specs=[hbm] * 5,
            out_specs=(vmem,) * 5,
            scratch_shapes=[
                pltpu.VMEM((halves, 3 * rows, width, LANES), f32),
                pltpu.VMEM((halves, 2 * rows, width, LANES), f32),
                pltpu.VMEM((halves, 2 * rows - 2, width, LANES), f32),
                pltpu.VMEM((halves - 1, rows, cols, LANES), f32),
                pltpu.VMEM((2 * rows + 1, width, LANES), f32),
                pltpu.VMEM((2 * rows, width, LANES), f32),
                pltpu.VMEM((2 * rows, width, LANES), f32),
                pltpu.VMEM((6, 2 * rows, cols), f32),
                pltpu.VMEM((width, LANES), f32),
                pltpu.VMEM((width, LANES), f32),
                pltpu.VMEM((width, LANES), f32),
                pltpu.VMEM((halves, n, TILE, LANES), f32),
                pltpu.SMEM(table.shape, f32),
                pltpu.VMEM(habitat.shape, jnp.int32),
                pltpu.VMEM((halves, LANES), jnp.int32),
                pltpu.VMEM((halves, LANES), jnp.int32),
                dma((4,)), dma((halves,)),
                dma((5,)), dma((halves,)), dma((halves, 2)), dma((halves, 2)),
                dma((halves, parts)), dma((halves, parts)),
                dma((halves, most)), dma((halves, most)),
                dma((halves,)), dma((3,)), dma((1,)), dma((2,)),
                dma((1,)), dma((1,)), dma((1,)), dma((1,)),
                pltpu.SemaphoreType.REGULAR((rounds,)),
            ],
            compiler_params=pltpu.CompilerParams(
                collective_id=0, has_side_effects=True, vmem_limit_bytes=32 * 2**20),
        )(*(pltpu.with_memory_space_constraint(value, pltpu.HBM) for value in (
            table, habitat, source_cell.reshape(halves, LANES),
            ground_cell.reshape(halves, LANES), start_potential)))
        potentials, residual, drop = pl.pallas_call(
            closing,
            out_shape=(field, field, drops),
            in_specs=[vmem] * 5,
            out_specs=(hbm,) * 3,
            scratch_shapes=[
                pltpu.VMEM((rows, cols, LANES), f32),
                pltpu.VMEM((rows, cols, LANES), f32),
                dma((3,)),
            ],
            compiler_params=pltpu.CompilerParams(vmem_limit_bytes=16 * 2**20),
        )(*stages)
        return potentials, residual, drop.reshape(rhs)

    placed = (
        P(("grp", "tile"), None, None),
        P(),
        P("grp"),
        P("grp"),
        P(("grp", "tile"), None, None, None),
    )
    return jax.shard_map(
        shards,
        mesh=mesh,
        in_specs=placed,
        out_specs=(placed[4], placed[4], P("grp")),
        check_vma=False,
    )
```

```python
import functools

import jax
import jax.numpy as jnp
from jax import lax
from jax.experimental import pallas as pl
from jax.experimental.pallas import tpu as pltpu
from jax.sharding import PartitionSpec as P

LANES = 128
TILE = 8
PAD = 2 * TILE
MESH = pl.DeviceIdType.MESH


def cuts(total, weights):
    bounds, seen = [0], 0
    for weight in weights:
        seen += weight
        bounds.append(total * seen // sum(weights))
    return bounds


def kernel(n, rows, cols, rounds, ahead, pass_weights, own_weights,
           table_hbm, habitat_hbm, source_hbm, ground_hbm, start_ref,
           pot_ref, res_ref, field_ref, coef_ref, drop_ref,
           X, R, W, U, V, H, D, C, T, TV, TH, S,
           table_ref, habitat_ref, source_ref, ground_ref, small_sem, load_sem,
           cond_recv, side_recv, edge_recv, cross_recv, pass_recv, relay_recv, near_recv,
           sum_recv, cond_send, side_send, cross_send, near_send, edge_send, far_send, relay_send, sum_send, hello):
    halves = X.shape[0]
    width = cols + 2 * PAD
    me = lax.axis_index("tile")
    chips = n // 2
    chip = me // 2
    core = me % 2
    odd = chip % 2
    side = me + 1 - 2 * core
    partner = me + 2 - 4 * odd
    diagonal = me - 2 + 4 * odd
    relay_to = me + 4 - 8 * odd
    relay_from = me - 4 + 8 * odd
    has_above = chip > 0
    has_below = chip < chips - 1
    has_diagonal = jnp.where(odd == 0, chip > 0, chip < chips - 1)
    can_relay = jnp.where(odd == 0, chip + 2 < chips, chip >= 2)
    gets_relay = jnp.where(odd == 0, chip >= 2, chip + 2 < chips)
    own = pl.ds(PAD, cols)
    body = cols // TILE - 1
    pass_at = [cuts(body, weights) for weights in pass_weights]
    pass_sem = cuts(sum(map(len, pass_weights)), list(map(len, pass_weights)))
    own_sem = cuts(sum(map(len, own_weights)), list(map(len, own_weights)))
    own_at = [cuts(body, weights) for weights in own_weights]

    def remote(src, dst, send, recv, target):
        return pltpu.make_async_remote_copy(
            src_ref=src, dst_ref=dst, send_sem=send, recv_sem=recv,
            device_id={"tile": target}, device_id_type=MESH)

    def arrived(place, recv):
        remote(place, place, near_send.at[0], recv, partner).wait_recv()

    def drained(place, send):
        remote(place, place, send, sum_recv.at[0], partner).wait_send()

    def signal(sem, target):
        pl.semaphore_signal(sem, inc=1, device_id={"tile": target}, device_id_type=MESH)

    def load(h):
        return pltpu.make_async_copy(
            start_ref.at[0, :, :, pl.ds(h * LANES, LANES)], X.at[h, pl.ds(rows, rows), own, :],
            load_sem.at[h])

    smalls = [
        pltpu.make_async_copy(src, dst, small_sem.at[k])
        for k, (src, dst) in enumerate((
            (table_hbm, table_ref), (habitat_hbm, habitat_ref),
            (source_hbm, source_ref), (ground_hbm, ground_ref)))
    ]

    barrier = pltpu.get_barrier_semaphore()
    signal(barrier, side)

    @pl.when(has_above)
    def _():
        signal(barrier, me - 2)
        signal(barrier, side - 2)

    @pl.when(has_below)
    def _():
        signal(barrier, me + 2)
        signal(barrier, side + 2)

    @pl.when(gets_relay)
    def _():
        signal(barrier, relay_from)

    for h in range(halves):
        load(h).start()
    for copy in smalls:
        copy.start()

    inner = pl.multiple_of(PAD + (1 - core) * (cols - TILE), TILE)
    outer = pl.multiple_of((1 - core) * TILE + core * (PAD + cols), TILE)
    halo = pl.multiple_of(core * TILE + (1 - core) * (PAD + cols), TILE)
    inner_at, outer_at, halo_at = pl.ds(inner, TILE), pl.ds(outer, TILE), pl.ds(halo, TILE)

    def span(bounds, j):
        start = pl.multiple_of(PAD + core * TILE + bounds[j] * TILE, TILE)
        return pl.ds(start, (bounds[j + 1] - bounds[j]) * TILE)

    def side_copy(h):
        place = pl.ds(rows, rows)
        return remote(X.at[h, place, inner_at, :], X.at[h, place, outer_at, :],
                      side_send.at[0], side_recv.at[h], side)

    def side_wait(h):
        arrived(X.at[h, pl.ds(rows, rows), halo_at, :], side_recv.at[h])

    def edge_near(h):
        return remote(X.at[h, pl.ds(rows + 1 - odd, rows - 1), inner_at, :],
                      X.at[h, pl.ds(odd * 2 * rows + 1 - odd, rows - 1), inner_at, :],
                      edge_send.at[0], edge_recv.at[h, 0], partner)

    def edge_far(h):
        return remote(X.at[h, pl.ds(rows + odd, rows - 1), inner_at, :],
                      X.at[h, pl.ds((1 - odd) * 2 * rows + odd, rows - 1), inner_at, :],
                      far_send.at[0], edge_recv.at[h, 1], diagonal)

    near_rows = pl.ds((1 - odd) * 2 * rows + odd, rows - 1)
    far_rows = pl.ds(odd * 2 * rows + 1 - odd, rows - 1)

    def cross(h, k):
        place = (near_rows, far_rows)[k]
        return remote(X.at[h, place, inner_at, :], X.at[h, place, outer_at, :],
                      cross_send.at[k], cross_recv.at[h, k], side)

    def cross_wait(h, k):
        arrived(X.at[h, (near_rows, far_rows)[k], halo_at, :], cross_recv.at[h, k])

    def pass_copy(h, j):
        at = span(pass_at[h], j)
        return remote(X.at[h, pl.ds(rows + odd, rows - 1), at, :],
                      X.at[h, pl.ds(odd * 2 * rows + odd, rows - 1), at, :],
                      near_send.at[0], pass_recv.at[pass_sem[h] + j], partner)

    def relay_copy(h, j):
        at = span(pass_at[h], j)
        return remote(X.at[h, pl.ds((1 - odd) * (2 * rows + 1), rows - 1), at, :],
                      X.at[h, far_rows, at, :],
                      relay_send.at[0], relay_recv.at[pass_sem[h] + j], relay_to)

    def near_copy(h, k):
        at = span(own_at[h], k)
        row = (1 - odd) * (rows - 1)
        return remote(X.at[h, rows + row, at, :], X.at[h, odd * 2 * rows + row, at, :],
                      near_send.at[0], near_recv.at[own_sem[h] + k], partner)

    for copy in smalls:
        copy.wait()
    cells = habitat_ref[0]
    cond = jnp.zeros(cells.shape, jnp.float32)
    for level in range(table_ref.shape[0]):
        cond = jnp.where(cells == level, table_ref[level], cond)
    C[5, 0:rows, :] = cond
    C[5, rows:2 * rows, :] = cond

    pl.semaphore_wait(
        barrier,
        1 + 2 * has_above.astype(jnp.int32) + 2 * has_below.astype(jnp.int32) + can_relay.astype(jnp.int32))

    def cond_copy(target, slot, kind):
        return remote(C.at[5], C.at[slot], cond_send.at[kind], cond_recv.at[slot], target)

    def inner_lanes(which):
        return pl.ds(pl.multiple_of(which * (cols - LANES), LANES), LANES)

    def corner_copy(target, slot, kind):
        at = inner_lanes(1 - core)
        return remote(C.at[5, :, at], C.at[slot, :, at], cond_send.at[kind], cond_recv.at[slot], target)

    def corner_wait(slot):
        arrived(C.at[slot, :, inner_lanes(core)], cond_recv.at[slot])

    cond_copy(side, 2, 0).start()

    @pl.when(has_above)
    def _():
        cond_copy(me - 2, 1, 1).start()
        corner_copy(side - 2, 4, 3).start()

    @pl.when(has_below)
    def _():
        cond_copy(me + 2, 0, 2).start()
        corner_copy(side + 2, 3, 4).start()

    for h in range(halves):
        load(h).wait()
        side_copy(h).start()
        edge_near(h).start()

        @pl.when(has_diagonal)
        def _():
            edge_far(h).start()

    parts = list(map(len, pass_weights))
    stream = []
    for h in range(halves):
        stream += [pass_copy(h, j) for j in range(parts[h])]
        stream += [near_copy(h, k) for k in range(len(own_weights[h]))]
    for copy in stream[:ahead]:
        copy.start()

    def zero(ref, h, c):
        ref[h, :, c:c + TILE, :] = jnp.zeros((ref.shape[1], TILE, LANES), jnp.float32)

    for h in range(halves):
        for c in (0, width - TILE):
            zero(X, h, c)
            zero(R, h, c)
            zero(W, h, c)

        @pl.when(core == 0)
        def _():
            zero(X, h, TILE)

        @pl.when(core == 1)
        def _():
            zero(X, h, width - PAD)

        @pl.when(jnp.logical_not(has_above))
        def _():
            X[h, 0:rows] = jnp.zeros((rows, width, LANES), jnp.float32)

        @pl.when(jnp.logical_not(has_below))
        def _():
            X[h, 2 * rows:3 * rows] = jnp.zeros((rows, width, LANES), jnp.float32)

    for h in range(halves):
        arrived(X.at[h, near_rows, inner_at, :], edge_recv.at[h, 0])
        cross(h, 0).start()

    @pl.when(has_diagonal)
    def _():
        for h in range(halves):
            arrived(X.at[h, far_rows, inner_at, :], edge_recv.at[h, 1])
            cross(h, 1).start()

    arrived(C.at[2], cond_recv.at[2])

    @pl.when(has_above)
    def _():
        arrived(C.at[0], cond_recv.at[0])
        corner_wait(3)

    @pl.when(has_below)
    def _():
        arrived(C.at[1], cond_recv.at[1])
        corner_wait(4)

    @pl.when(jnp.logical_not(has_above))
    def _():
        for slot in (0, 3):
            C[slot] = jnp.zeros(C.shape[1:], jnp.float32)

    @pl.when(jnp.logical_not(has_below))
    def _():
        for slot in (1, 4):
            C[slot] = jnp.zeros(C.shape[1:], jnp.float32)

    def greet(r):
        d = 2 << r

        @pl.when(me >= d)
        def _():
            signal(hello.at[r], me - d)

        @pl.when(me + d < n)
        def _():
            signal(hello.at[r], me + d)

    def greeted(r):
        d = 2 << r
        pl.semaphore_wait(hello.at[r], (me >= d).astype(jnp.int32) + (me + d < n).astype(jnp.int32))

    for copy in stream[ahead:]:
        copy.start()
    greet(0)

    first = lax.broadcasted_iota(jnp.int32, (2 * rows, LANES), 0) < rows

    def turned(above, here, below, j):
        lanes = slice(j * LANES, (j + 1) * LANES)
        top = jnp.where(first, C[above, :, lanes], C[here, :, lanes])
        blank = jnp.zeros((LANES - 4 * rows, LANES), jnp.float32)
        return jnp.transpose(jnp.concatenate([top, C[below, :, lanes], blank], 0))

    for j in range(cols // LANES):
        T[PAD + j * LANES:PAD + (j + 1) * LANES, :] = turned(0, 5, 1, j)
    for c in (0, TILE, width - PAD, width - TILE):
        T[c:c + TILE, :] = jnp.zeros((TILE, LANES), jnp.float32)

    @pl.when(core == 0)
    def _():
        T[width - PAD:width - TILE, :] = turned(3, 2, 4, 0)[0:TILE]

    @pl.when(core == 1)
    def _():
        T[TILE:PAD, :] = turned(3, 2, 4, cols // LANES - 1)[LANES - TILE:]

    def global_col(c):
        return core * cols - PAD + c + lax.broadcasted_iota(jnp.int32, (TILE, LANES), 0)

    global_row = chip * rows - rows + lax.broadcasted_iota(jnp.int32, (TILE, LANES), 1)
    total_rows, total_cols = chips * rows, 2 * cols

    def edges(t, _):
        c = pl.multiple_of(t * TILE, TILE)
        here = T[pl.ds(c, TILE), :]
        east = T[pl.ds(c + 1, TILE), :]
        south = pltpu.roll(here, LANES - 1, 1)
        gc = global_col(c)
        in_row = (global_row >= 0) & (global_row < total_rows - 1)
        TV[pl.ds(c, TILE), :] = jnp.where(in_row, 0.5 * (here + south), 0.0)
        in_col = (gc >= 0) & (gc < total_cols - 1)
        TH[pl.ds(c, TILE), :] = jnp.where(in_col, 0.5 * (here + east), 0.0)
        return 0

    TH[0:TILE, :] = jnp.zeros((TILE, LANES), jnp.float32)
    H[:, 0:TILE, :] = jnp.zeros((H.shape[0], TILE, LANES), jnp.float32)
    lax.fori_loop(1, width // TILE - 1, edges, 0, unroll=6)

    def spread(t, _):
        c = pl.multiple_of(t * TILE, TILE)
        at = pl.ds(c, TILE)
        v = TV[at, :]
        east = TH[at, :]
        west = TH[pl.ds(c - 1, TILE), :]
        diag = v + pltpu.roll(v, 1, 1) + east + west
        shape = (TILE, LANES)
        for k in range(2 * rows + 1):
            V[k, at, :] = jnp.broadcast_to(v[:, k + 1:k + 2], shape)
        for k in range(2 * rows):
            H[k, at, :] = jnp.broadcast_to(east[:, k + 2:k + 3], shape)
            D[k, at, :] = jnp.broadcast_to(diag[:, k + 2:k + 3], shape)
        return 0

    tiles = width // TILE

    def relay(h, j):
        arrived(X.at[h, pl.ds((1 - odd) * (2 * rows + 1), rows - 1), span(pass_at[h], j), :],
                pass_recv.at[pass_sem[h] + j])

        @pl.when(can_relay)
        def _():
            relay_copy(h, j).start()

    splits = cuts(tiles - 2, [1] * parts[0])
    for j in range(parts[0]):
        lax.fori_loop(1 + splits[j], 1 + splits[j + 1], spread, 0)
        relay(0, j)
        if j < rounds:
            greeted(j)
            if j + 1 < rounds:
                greet(j + 1)
    for j in range(parts[0], rounds):
        greeted(j)
        if j + 1 < rounds:
            greet(j + 1)

    def shape_of(cells, h, top):
        base = (chip * rows + top) * total_cols + core * cols - PAD
        return jnp.broadcast_to(cells[h:h + 1, :] - base, (TILE, LANES))

    def applied(ref, h, skip, count, c, low, grounds):
        at = pl.ds(c, TILE)
        west = pl.ds(c - 1, TILE)
        east = pl.ds(c + 1, TILE)
        column = c + lax.broadcasted_iota(jnp.int32, (TILE, LANES), 0)
        mid = ref[h, skip + 1, at, :]
        flow = V[low, at, :] * ref[h, skip, at, :]
        for k in range(count):
            after = ref[h, skip + k + 2, at, :]
            v = V[low + k + 1, at, :]
            grounded = column == grounds[k]
            diag = D[low + k, at, :]
            out = jnp.where(grounded, diag + 1.0, diag) * mid - flow
            out = out - v * after
            out = out - H[low + k, west, :] * ref[h, skip + 1 + k, west, :]
            out = out - H[low + k, at, :] * ref[h, skip + 1 + k, east, :]
            yield k, out, mid, grounded, column
            flow = v * mid
            mid = after

    def zeros():
        return tuple(jnp.zeros((TILE, LANES), jnp.float32) for _ in range(7))

    def compute(h, j, acc):
        def named(cells, top, count):
            return [shape_of(cells, h, top + k) for k in range(count)]

        count_r, count_w = 2 * rows, 2 * rows - 2
        src_r, gnd_r = named(source_ref, -2, count_r), named(ground_ref, -2, count_r)
        gnd_w = named(ground_ref, -1, count_w)
        src_u, gnd_u = named(source_ref, 0, rows), named(ground_ref, 0, rows)

        def pass_r(t, _):
            c = pl.multiple_of(t * TILE, TILE)
            for k, a, _mid, _g, column in applied(X, h, 1, count_r, c, 0, gnd_r):
                R[h, k, pl.ds(c, TILE), :] = jnp.where(column == src_r[k], 1.0 - a, -a)
            return 0

        def pass_w(t, _):
            c = pl.multiple_of(t * TILE, TILE)
            for k, a, _mid, _g, _column in applied(R, h, 0, count_w, c, 1, gnd_w):
                W[h, k, pl.ds(c, TILE), :] = a
            return 0

        def pass_u(t, acc):
            c = pl.multiple_of(t * TILE, TILE)
            at = pl.ds(c, TILE)
            to = pl.ds(c - PAD, TILE)
            for k, u, w, grounded, column in applied(W, h, 0, rows, c, 2, gnd_u):
                r = R[h, 2 + k, at, :]
                x = X[h, rows + k, at, :]
                if h < halves - 1:
                    U[h, k, to, :] = u
                else:
                    for place, value in enumerate((x, r, w, u)):
                        field_ref[place, k, to, :] = value
                sign = jnp.where(column == src_u[k], 1.0, 0.0) - jnp.where(grounded, 1.0, 0.0)
                terms = (r * r, r * w, w * w, w * u, sign * x, sign * r, sign * w)
                acc = tuple(s + term for s, term in zip(acc, terms))
            return acc

        def sweep(lag, step, carry):
            bounds = own_at[h]
            begin, end = (1, tiles - 1) if lag < 3 else (2, tiles - 2)
            offset = PAD // TILE - lag
            final = j == len(bounds) - 2
            start = begin if j == 0 else offset + core + bounds[j]
            count = (end - 1 if final else offset + bounds[j + 1]) - (begin if j == 0 else offset + bounds[j])
            extra = core if j == 0 else 1 - core if final else None
            pairs = count // 2

            def pair(i, carry):
                return step(start + 2 * i + 1, step(start + 2 * i, carry))

            carry = lax.fori_loop(0, pairs, pair, carry)
            if count % 2:
                carry = step(start + 2 * pairs, carry)
            if extra is not None and not (j == 0 and final):
                carry = lax.fori_loop(start + count, start + count + extra, step, carry)
            return carry

        sweep(1, pass_r, 0)
        sweep(2, pass_w, 0)
        return sweep(3, pass_u, acc)

    def sum_copy(h, d):
        return remote(S.at[h, me], S.at[h, me], sum_send.at[0], sum_recv.at[h], (me + d) % n)

    def send_sums(h, acc):
        sums = [jnp.sum(s, axis=0, keepdims=True) for s in acc]
        S[h, me] = jnp.concatenate(sums + [jnp.zeros((1, LANES), jnp.float32)], 0)
        lax.fori_loop(1, n, lambda d, _: (sum_copy(h, d).start(), 0)[1], 0)

    def totals(h):
        arrived(S.at[h, pl.ds(0, n - 1)], sum_recv.at[h])
        total = S[h, 0]
        for k in range(1, n):
            total = total + S[h, k]
        m0, m1, m2, m3, ex, er, ew = (total[k:k + 1] for k in range(7))
        a0 = m0 / m1
        next_norm = a0 * (a0 * m2 - m1)
        ratio = next_norm / m0
        curve = m1 - a0 * (2.0 * m2 - a0 * m3)
        a1 = next_norm / (curve - ratio * next_norm / a0)
        p = a0 + a1 * (1.0 + ratio)
        q = a1 * a0
        drop_ref[h:h + 1, :] = ex + p * er - q * ew
        return p, q

    def finish(h):
        p, q = totals(h)
        p1 = jnp.broadcast_to(p, (TILE, LANES))
        q1 = jnp.broadcast_to(q, (TILE, LANES))

        def last(t, _):
            c = pl.multiple_of(t * TILE, TILE)
            at = pl.ds(c + PAD, TILE)
            to = pl.ds(c, TILE)
            for k in range(rows):
                r = R[h, 2 + k, at, :]
                w = W[h, 1 + k, at, :]
                pot_ref[h, k, to, :] = X[h, rows + k, at, :] + p1 * r - q1 * w
                res_ref[h, k, to, :] = r - p1 * w + q1 * U[h, k, to, :]
            return 0

        lax.fori_loop(0, cols // TILE, last, 0)

    for h in range(halves):
        side_wait(h)
        cross_wait(h, 0)

        @pl.when(has_diagonal)
        def _():
            cross_wait(h, 1)

        acc = zeros()
        relayed = 0
        for k in range(len(own_weights[h])):
            while relayed < parts[h] and pass_at[h][relayed] < own_at[h][k + 1]:
                @pl.when(gets_relay)
                def _():
                    arrived(X.at[h, far_rows, span(pass_at[h], relayed), :], relay_recv.at[pass_sem[h] + relayed])
                relayed += 1

            arrived(X.at[h, (1 - odd) * 2 * rows + odd * (rows - 1), span(own_at[h], k), :],
                    near_recv.at[own_sem[h] + k])
            acc = compute(h, k, acc)
        send_sums(h, acc)
        if h < halves - 1:
            for j in range(parts[h + 1]):
                relay(h + 1, j)

    for h in range(halves - 1):
        finish(h)

    p, q = totals(halves - 1)
    coef_ref[...] = jnp.concatenate([p, q, jnp.zeros((TILE - 2, LANES), jnp.float32)], 0)

    drained(C.at[0], cond_send.at[0])

    @pl.when(has_above)
    def _():
        drained(C.at[0], cond_send.at[1])
        drained(C.at[0, :, pl.ds(0, LANES)], cond_send.at[3])

    @pl.when(has_below)
    def _():
        drained(C.at[0], cond_send.at[2])
        drained(C.at[0, :, pl.ds(0, LANES)], cond_send.at[4])

    drained(X.at[:, pl.ds(0, rows), pl.ds(0, TILE), :], side_send.at[0])
    drained(X.at[:, pl.ds(0, rows - 1), pl.ds(0, TILE), :], cross_send.at[0])
    drained(X.at[:, pl.ds(0, rows - 1), pl.ds(0, TILE), :], edge_send.at[0])
    drained(X.at[:, pl.ds(0, rows), pl.ds(0, cols - TILE), :], near_send.at[0])

    @pl.when(has_diagonal)
    def _():
        drained(X.at[:, pl.ds(0, rows - 1), pl.ds(0, TILE), :], cross_send.at[1])
        drained(X.at[:, pl.ds(0, rows - 1), pl.ds(0, TILE), :], far_send.at[0])

    @pl.when(can_relay)
    def _():
        drained(X.at[:, pl.ds(0, rows - 1), pl.ds(0, cols - TILE), :], relay_send.at[0])

    drained(S.at[:, pl.ds(0, n - 1)], sum_send.at[0])


def closing(pot_ref, res_ref, field_ref, coef_ref, drop_ref, pot_out, res_out, drop_out,
            P1, Q1, sem):
    rows, cols = field_ref.shape[1], field_ref.shape[2]
    before = pot_ref.shape[0]

    def put(ref, out, h, c, count, k):
        return pltpu.make_async_copy(
            ref.at[:, pl.ds(c, count), :],
            out.at[0, :, pl.ds(c, count), pl.ds(h * LANES, LANES)], sem.at[k])

    for h in range(before):
        put(pot_ref.at[h], pot_out, h, 0, cols, 0).start()
        put(res_ref.at[h], res_out, h, 0, cols, 1).start()
    drop = pltpu.make_async_copy(drop_ref, drop_out, sem.at[2])
    drop.start()

    p1 = jnp.broadcast_to(coef_ref[0:1, :], (TILE, LANES))
    q1 = jnp.broadcast_to(coef_ref[1:2, :], (TILE, LANES))
    pieces = 4
    step = cols // pieces

    def last(t, _):
        c = pl.multiple_of(t * TILE, TILE)
        at = pl.ds(c, TILE)
        for k in range(rows):
            x, r, w, u = (field_ref[place, k, at, :] for place in range(4))
            P1[k, at, :] = x + p1 * r - q1 * w
            Q1[k, at, :] = r - p1 * w + q1 * u
        return 0

    for piece in range(pieces):
        lax.fori_loop(piece * step // TILE, (piece + 1) * step // TILE, last, 0, unroll=2)
        put(P1, pot_out, before, piece * step, step, 0).start()
        put(Q1, res_out, before, piece * step, step, 1).start()

    for k, out in enumerate((pot_out, res_out)):
        pltpu.make_async_copy(out, out, sem.at[k]).wait()
    drop.wait()


def solution(mesh):
    n = mesh.shape["tile"]
    rounds = max(1, (n // 2 - 1).bit_length())

    def shards(habitat, table, source_cell, ground_cell, start_potential):
        _, rows, cols, rhs = start_potential.shape
        halves = rhs // LANES
        width = cols + 2 * PAD
        f32 = jnp.float32
        dma = pltpu.SemaphoreType.DMA
        field = jax.ShapeDtypeStruct(start_potential.shape, f32)
        part = jax.ShapeDtypeStruct((halves - 1, rows, cols, LANES), f32)
        drops = jax.ShapeDtypeStruct((halves, LANES), f32)
        vmem = pl.BlockSpec(memory_space=pltpu.VMEM)
        hbm = pl.BlockSpec(memory_space=pltpu.HBM)
        pass_weights = ((16, 16, 16, 15),) * (halves - 1) + ((12, 12, 12, 12, 8, 7),)
        own_weights = ((32, 31),) * (halves - 1) + ((9, 9, 9, 9, 9, 8, 6, 4),)
        passes, owns = sum(map(len, pass_weights)), sum(map(len, own_weights))
        stages = pl.pallas_call(
            functools.partial(kernel, n, rows, cols, rounds, 3, pass_weights, own_weights),
            out_shape=(part, part, jax.ShapeDtypeStruct((4, rows, cols, LANES), f32),
                       jax.ShapeDtypeStruct((TILE, LANES), f32), drops),
            in_specs=[hbm] * 5,
            out_specs=(vmem,) * 5,
            scratch_shapes=[
                pltpu.VMEM((halves, 3 * rows, width, LANES), f32),
                pltpu.VMEM((halves, 2 * rows, width, LANES), f32),
                pltpu.VMEM((halves, 2 * rows - 2, width, LANES), f32),
                pltpu.VMEM((halves - 1, rows, cols, LANES), f32),
                pltpu.VMEM((2 * rows + 1, width, LANES), f32),
                pltpu.VMEM((2 * rows, width, LANES), f32),
                pltpu.VMEM((2 * rows, width, LANES), f32),
                pltpu.VMEM((6, 2 * rows, cols), f32),
                pltpu.VMEM((width, LANES), f32),
                pltpu.VMEM((width, LANES), f32),
                pltpu.VMEM((width, LANES), f32),
                pltpu.VMEM((halves, n, TILE, LANES), f32),
                pltpu.SMEM(table.shape, f32),
                pltpu.VMEM(habitat.shape, jnp.int32),
                pltpu.VMEM((halves, LANES), jnp.int32),
                pltpu.VMEM((halves, LANES), jnp.int32),
                dma((4,)), dma((halves,)),
                dma((5,)), dma((halves,)), dma((halves, 2)), dma((halves, 2)),
                dma((passes,)), dma((passes,)), dma((owns,)),
                dma((halves,)), dma((5,)), dma((1,)), dma((2,)),
                dma((1,)), dma((1,)), dma((1,)), dma((1,)), dma((1,)),
                pltpu.SemaphoreType.REGULAR((rounds,)),
            ],
            compiler_params=pltpu.CompilerParams(
                collective_id=0, has_side_effects=True, vmem_limit_bytes=32 * 2**20),
        )(*(pltpu.with_memory_space_constraint(value, pltpu.HBM) for value in (
            table, habitat, source_cell.reshape(halves, LANES),
            ground_cell.reshape(halves, LANES), start_potential)))
        potentials, residual, drop = pl.pallas_call(
            closing,
            out_shape=(field, field, drops),
            in_specs=[vmem] * 5,
            out_specs=(hbm,) * 3,
            scratch_shapes=[
                pltpu.VMEM((rows, cols, LANES), f32),
                pltpu.VMEM((rows, cols, LANES), f32),
                dma((3,)),
            ],
            compiler_params=pltpu.CompilerParams(vmem_limit_bytes=16 * 2**20),
        )(*stages)
        return potentials, residual, drop.reshape(rhs)

    placed = (
        P(("grp", "tile"), None, None),
        P(),
        P("grp"),
        P("grp"),
        P(("grp", "tile"), None, None, None),
    )
    return jax.shard_map(
        shards,
        mesh=mesh,
        in_specs=placed,
        out_specs=(placed[4], placed[4], P("grp")),
        check_vma=False,
    )
```

```python
import functools

import jax
import jax.numpy as jnp
from jax import lax
from jax.experimental import pallas as pl
from jax.experimental.pallas import tpu as pltpu
from jax.sharding import PartitionSpec as P

LANES = 128
TILE = 8
PAD = 2 * TILE
MESH = pl.DeviceIdType.MESH


def cuts(total, weights):
    bounds, seen = [0], 0
    for weight in weights:
        seen += weight
        bounds.append(total * seen // sum(weights))
    return bounds


def kernel(n, rows, cols, rounds, pass_weights, own_weights,
           table_hbm, habitat_hbm, source_hbm, ground_hbm, start_ref,
           pot_ref, res_ref, field_ref, coef_ref, drop_ref,
           X, R, W, U, V, H, D, C, T, TV, TH, S,
           table_ref, habitat_ref, source_ref, ground_ref, small_sem, load_sem,
           cond_recv, side_recv, edge_recv, cross_recv, pass_recv, relay_recv, third_recv, help_recv, far_recv, near_recv,
           sum_recv, cond_send, side_send, cross_send, near_send, edge_send, far_send, relay_send, pass_send, third_send, onward_send, forward_send, sum_send, hello):
    halves = X.shape[0]
    width = cols + 2 * PAD
    me = lax.axis_index("tile")
    chips = n // 2
    chip = me // 2
    core = me % 2
    odd = chip % 2
    side = me + 1 - 2 * core
    partner = me + 2 - 4 * odd
    diagonal = me - 2 + 4 * odd
    relay_to = me + 4 - 8 * odd
    relay_from = me - 4 + 8 * odd
    has_above = chip > 0
    has_below = chip < chips - 1
    has_diagonal = jnp.where(odd == 0, chip > 0, chip < chips - 1)
    can_relay = jnp.where(odd == 0, chip + 2 < chips, chip >= 2)
    gets_relay = jnp.where(odd == 0, chip >= 2, chip + 2 < chips)
    own = pl.ds(PAD, cols)
    body = cols // TILE - 1
    pass_at = [cuts(body, weights) for weights in pass_weights]
    pass_sem = cuts(sum(map(len, pass_weights)), list(map(len, pass_weights)))
    own_sem = cuts(sum(map(len, own_weights)), list(map(len, own_weights)))
    own_at = [cuts(body, weights) for weights in own_weights]

    def remote(src, dst, send, recv, target):
        return pltpu.make_async_remote_copy(
            src_ref=src, dst_ref=dst, send_sem=send, recv_sem=recv,
            device_id={"tile": target}, device_id_type=MESH)

    def arrived(place, recv):
        remote(place, place, near_send.at[0], recv, partner).wait_recv()

    def drained(place, send):
        remote(place, place, send, sum_recv.at[0], partner).wait_send()

    def signal(sem, target):
        pl.semaphore_signal(sem, inc=1, device_id={"tile": target}, device_id_type=MESH)

    def load(h):
        return pltpu.make_async_copy(
            start_ref.at[0, :, :, pl.ds(h * LANES, LANES)], X.at[h, pl.ds(rows, rows), own, :],
            load_sem.at[h])

    smalls = [
        pltpu.make_async_copy(src, dst, small_sem.at[k])
        for k, (src, dst) in enumerate((
            (table_hbm, table_ref), (habitat_hbm, habitat_ref),
            (source_hbm, source_ref), (ground_hbm, ground_ref)))
    ]

    barrier = pltpu.get_barrier_semaphore()
    signal(barrier, side)

    @pl.when(has_above)
    def _():
        signal(barrier, me - 2)
        signal(barrier, side - 2)

    @pl.when(has_below)
    def _():
        signal(barrier, me + 2)
        signal(barrier, side + 2)

    @pl.when(gets_relay)
    def _():
        signal(barrier, relay_from)

    @pl.when(can_relay)
    def _():
        signal(barrier, relay_to)

    for h in range(halves):
        load(h).start()
    for copy in smalls:
        copy.start()

    inner = pl.multiple_of(PAD + (1 - core) * (cols - TILE), TILE)
    outer = pl.multiple_of((1 - core) * TILE + core * (PAD + cols), TILE)
    halo = pl.multiple_of(core * TILE + (1 - core) * (PAD + cols), TILE)
    inner_at, outer_at, halo_at = pl.ds(inner, TILE), pl.ds(outer, TILE), pl.ds(halo, TILE)

    def span(bounds, j):
        start = pl.multiple_of(PAD + core * TILE + bounds[j] * TILE, TILE)
        return pl.ds(start, (bounds[j + 1] - bounds[j]) * TILE)

    def side_copy(h):
        place = pl.ds(rows, rows)
        return remote(X.at[h, place, inner_at, :], X.at[h, place, outer_at, :],
                      side_send.at[0], side_recv.at[h], side)

    def side_wait(h):
        arrived(X.at[h, pl.ds(rows, rows), halo_at, :], side_recv.at[h])

    def edge_near(h):
        return remote(X.at[h, pl.ds(rows + 1 - odd, rows - 1), inner_at, :],
                      X.at[h, pl.ds(odd * 2 * rows + 1 - odd, rows - 1), inner_at, :],
                      edge_send.at[0], edge_recv.at[h, 0], partner)

    def edge_far(h):
        return remote(X.at[h, pl.ds(rows + odd, rows - 1), inner_at, :],
                      X.at[h, pl.ds((1 - odd) * 2 * rows + odd, rows - 1), inner_at, :],
                      far_send.at[0], edge_recv.at[h, 1], diagonal)

    near_rows = pl.ds((1 - odd) * 2 * rows + odd, rows - 1)
    far_rows = pl.ds(odd * 2 * rows + 1 - odd, rows - 1)

    def cross(h, k):
        place = (near_rows, far_rows)[k]
        return remote(X.at[h, place, inner_at, :], X.at[h, place, outer_at, :],
                      cross_send.at[k], cross_recv.at[h, k], side)

    def cross_wait(h, k):
        arrived(X.at[h, (near_rows, far_rows)[k], halo_at, :], cross_recv.at[h, k])

    rank = jnp.where(odd == 0, chip // 2, chips // 2 - 1 - chip // 2)
    pairs, tally = chips // 2, halves * body

    def detours(k, h, j):
        return (pairs - k) * 2 * tally > pairs * (2 * h * body + pass_at[h][j] + pass_at[h][j + 1])

    def can_detour(h, j):
        return pairs > 1 and detours(1, h, j)

    outward = rows + odd * (rows - 1)
    lent = odd * (3 * rows - 1)
    guest = (1 - odd) * (3 * rows - 1)
    far_row = odd * 2 * rows + (1 - odd) * (rows - 1)
    far_there = (1 - odd) * 2 * rows + odd * (rows - 1)

    def pass_copy(h, j):
        at = span(pass_at[h], j)
        return remote(X.at[h, pl.ds(rows + 1, rows - 2), at, :],
                      X.at[h, pl.ds(odd * 2 * rows + 1, rows - 2), at, :],
                      pass_send.at[0], pass_recv.at[pass_sem[h] + j], partner)

    def relay_copy(h, j):
        at = span(pass_at[h], j)
        return remote(X.at[h, pl.ds((1 - odd) * 2 * rows + 1, rows - 2), at, :],
                      X.at[h, pl.ds(odd * 2 * rows + 1, rows - 2), at, :],
                      relay_send.at[0], relay_recv.at[pass_sem[h] + j], relay_to)

    def third_copy(h, j):
        at = span(pass_at[h], j)
        return remote(X.at[h, outward, at, :], X.at[h, odd * (3 * rows - 1), at, :],
                      third_send.at[0], third_recv.at[pass_sem[h] + j], partner)

    def help_copy(h, j):
        at = span(pass_at[h], j)
        return remote(X.at[h, outward, at, :], X.at[h, lent, at, :],
                      third_send.at[0], help_recv.at[pass_sem[h] + j], relay_from)

    def onward_copy(h, j):
        at = span(pass_at[h], j)
        return remote(X.at[h, guest, at, :], X.at[h, far_row, at, :],
                      onward_send.at[pass_sem[h] + j], far_recv.at[pass_sem[h] + j], relay_to)

    def forward_copy(h, j):
        at = span(pass_at[h], j)
        return remote(X.at[h, lent, at, :], X.at[h, far_there, at, :],
                      forward_send.at[pass_sem[h] + j], far_recv.at[pass_sem[h] + j], partner)

    def near_copy(h, k):
        at = span(own_at[h], k)
        row = (1 - odd) * (rows - 1)
        return remote(X.at[h, rows + row, at, :], X.at[h, odd * 2 * rows + row, at, :],
                      near_send.at[0], near_recv.at[own_sem[h] + k], partner)

    for copy in smalls:
        copy.wait()
    cells = habitat_ref[0]
    cond = jnp.zeros(cells.shape, jnp.float32)
    for level in range(table_ref.shape[0]):
        cond = jnp.where(cells == level, table_ref[level], cond)
    C[5, 0:rows, :] = cond
    C[5, rows:2 * rows, :] = cond

    pl.semaphore_wait(
        barrier,
        1 + 2 * has_above.astype(jnp.int32) + 2 * has_below.astype(jnp.int32)
        + can_relay.astype(jnp.int32) + gets_relay.astype(jnp.int32))

    def cond_copy(target, slot, kind):
        return remote(C.at[5], C.at[slot], cond_send.at[kind], cond_recv.at[slot], target)

    def inner_lanes(which):
        return pl.ds(pl.multiple_of(which * (cols - LANES), LANES), LANES)

    def corner_copy(target, slot, kind):
        at = inner_lanes(1 - core)
        return remote(C.at[5, :, at], C.at[slot, :, at], cond_send.at[kind], cond_recv.at[slot], target)

    def corner_wait(slot):
        arrived(C.at[slot, :, inner_lanes(core)], cond_recv.at[slot])

    cond_copy(side, 2, 0).start()

    @pl.when(has_above)
    def _():
        cond_copy(me - 2, 1, 1).start()
        corner_copy(side - 2, 4, 3).start()

    @pl.when(has_below)
    def _():
        cond_copy(me + 2, 0, 2).start()
        corner_copy(side + 2, 3, 4).start()

    for h in range(halves):
        load(h).wait()
        side_copy(h).start()
        edge_near(h).start()

        @pl.when(has_diagonal)
        def _():
            edge_far(h).start()

    parts = list(map(len, pass_weights))

    for h in range(halves):
        for j in range(parts[h]):
            if can_detour(h, j):
                @pl.when(gets_relay & detours(rank, h, j))
                def _():
                    help_copy(h, j).start()

    def send_pass(h, j):
        pass_copy(h, j).start()

        @pl.when(gets_relay & jnp.logical_not(detours(rank, h, j)))
        def _():
            third_copy(h, j).start()

    def send_rest(h, done):
        for j in range(done, parts[h]):
            send_pass(h, j)
        for k in range(len(own_weights[h])):
            near_copy(h, k).start()

    send_pass(0, 0)

    def zero(ref, h, c):
        ref[h, :, c:c + TILE, :] = jnp.zeros((ref.shape[1], TILE, LANES), jnp.float32)

    for h in range(halves):
        for c in (0, width - TILE):
            zero(X, h, c)
            zero(R, h, c)
            zero(W, h, c)

        @pl.when(core == 0)
        def _():
            zero(X, h, TILE)

        @pl.when(core == 1)
        def _():
            zero(X, h, width - PAD)

        @pl.when(jnp.logical_not(has_above))
        def _():
            X[h, 1:rows] = jnp.zeros((rows - 1, width, LANES), jnp.float32)

        @pl.when(jnp.logical_not(has_below))
        def _():
            X[h, 2 * rows:3 * rows - 1] = jnp.zeros((rows - 1, width, LANES), jnp.float32)

    for h in range(halves):
        arrived(X.at[h, near_rows, inner_at, :], edge_recv.at[h, 0])
        cross(h, 0).start()

    @pl.when(has_diagonal)
    def _():
        for h in range(halves):
            arrived(X.at[h, far_rows, inner_at, :], edge_recv.at[h, 1])
            cross(h, 1).start()

    arrived(C.at[2], cond_recv.at[2])

    @pl.when(has_above)
    def _():
        arrived(C.at[0], cond_recv.at[0])
        corner_wait(3)

    @pl.when(has_below)
    def _():
        arrived(C.at[1], cond_recv.at[1])
        corner_wait(4)

    @pl.when(jnp.logical_not(has_above))
    def _():
        for slot in (0, 3):
            C[slot] = jnp.zeros(C.shape[1:], jnp.float32)

    @pl.when(jnp.logical_not(has_below))
    def _():
        for slot in (1, 4):
            C[slot] = jnp.zeros(C.shape[1:], jnp.float32)

    def greet(r):
        d = 2 << r

        @pl.when(me >= d)
        def _():
            signal(hello.at[r], me - d)

        @pl.when(me + d < n)
        def _():
            signal(hello.at[r], me + d)

    def greeted(r):
        d = 2 << r
        pl.semaphore_wait(hello.at[r], (me >= d).astype(jnp.int32) + (me + d < n).astype(jnp.int32))

    send_rest(0, 1)
    greet(0)

    first = lax.broadcasted_iota(jnp.int32, (2 * rows, LANES), 0) < rows

    def turned(above, here, below, j):
        lanes = slice(j * LANES, (j + 1) * LANES)
        top = jnp.where(first, C[above, :, lanes], C[here, :, lanes])
        blank = jnp.zeros((LANES - 4 * rows, LANES), jnp.float32)
        return jnp.transpose(jnp.concatenate([top, C[below, :, lanes], blank], 0))

    for j in range(cols // LANES):
        T[PAD + j * LANES:PAD + (j + 1) * LANES, :] = turned(0, 5, 1, j)
    for c in (0, TILE, width - PAD, width - TILE):
        T[c:c + TILE, :] = jnp.zeros((TILE, LANES), jnp.float32)

    @pl.when(core == 0)
    def _():
        T[width - PAD:width - TILE, :] = turned(3, 2, 4, 0)[0:TILE]

    @pl.when(core == 1)
    def _():
        T[TILE:PAD, :] = turned(3, 2, 4, cols // LANES - 1)[LANES - TILE:]

    def global_col(c):
        return core * cols - PAD + c + lax.broadcasted_iota(jnp.int32, (TILE, LANES), 0)

    global_row = chip * rows - rows + lax.broadcasted_iota(jnp.int32, (TILE, LANES), 1)
    total_rows, total_cols = chips * rows, 2 * cols

    def edges(t, _):
        c = pl.multiple_of(t * TILE, TILE)
        here = T[pl.ds(c, TILE), :]
        east = T[pl.ds(c + 1, TILE), :]
        south = pltpu.roll(here, LANES - 1, 1)
        gc = global_col(c)
        in_row = (global_row >= 0) & (global_row < total_rows - 1)
        TV[pl.ds(c, TILE), :] = jnp.where(in_row, 0.5 * (here + south), 0.0)
        in_col = (gc >= 0) & (gc < total_cols - 1)
        TH[pl.ds(c, TILE), :] = jnp.where(in_col, 0.5 * (here + east), 0.0)
        return 0

    TH[0:TILE, :] = jnp.zeros((TILE, LANES), jnp.float32)
    H[:, 0:TILE, :] = jnp.zeros((H.shape[0], TILE, LANES), jnp.float32)
    lax.fori_loop(1, width // TILE - 1, edges, 0, unroll=6)

    def spread(t, _):
        c = pl.multiple_of(t * TILE, TILE)
        at = pl.ds(c, TILE)
        v = TV[at, :]
        east = TH[at, :]
        west = TH[pl.ds(c - 1, TILE), :]
        diag = v + pltpu.roll(v, 1, 1) + east + west
        shape = (TILE, LANES)
        for k in range(2 * rows + 1):
            V[k, at, :] = jnp.broadcast_to(v[:, k + 1:k + 2], shape)
        for k in range(2 * rows):
            H[k, at, :] = jnp.broadcast_to(east[:, k + 2:k + 3], shape)
            D[k, at, :] = jnp.broadcast_to(diag[:, k + 2:k + 3], shape)
        return 0

    tiles = width // TILE

    def relay(h, j):
        arrived(X.at[h, pl.ds((1 - odd) * 2 * rows + 1, rows - 2), span(pass_at[h], j), :],
                pass_recv.at[pass_sem[h] + j])

        @pl.when(can_relay)
        def _():
            relay_copy(h, j).start()

    def onward(h, j):
        @pl.when(can_relay & jnp.logical_not(detours(pairs - 1 - rank, h, j)))
        def _():
            arrived(X.at[h, guest, span(pass_at[h], j), :], third_recv.at[pass_sem[h] + j])
            onward_copy(h, j).start()

    def forward(h, j):
        if can_detour(h, j):
            @pl.when(can_relay & detours(rank + 1, h, j))
            def _():
                arrived(X.at[h, lent, span(pass_at[h], j), :], help_recv.at[pass_sem[h] + j])
                forward_copy(h, j).start()

    def meet(r):
        if r < rounds:
            greeted(r)
            if r + 1 < rounds:
                greet(r + 1)

    steps = [[lambda j=j: relay(0, j), lambda j=j: onward(0, j)] for j in range(parts[0])]
    steps = sum(steps, [])
    lends = [(h, j) for h in range(halves) for j in range(parts[h])]
    splits = cuts(tiles - 2, [1] * len(steps))
    for i, step in enumerate(steps):
        lax.fori_loop(1 + splits[i], 1 + splits[i + 1], spread, 0)
        step()
        meet(i)
        if i == 0:
            for j in range(parts[0]):
                forward(0, j)
        if i == 1:
            for h, j in lends[parts[0]:]:
                forward(h, j)
            for h in range(1, halves):
                send_rest(h, 0)
    for r in range(len(steps), rounds):
        meet(r)

    def shape_of(cells, h, top):
        base = (chip * rows + top) * total_cols + core * cols - PAD
        return jnp.broadcast_to(cells[h:h + 1, :] - base, (TILE, LANES))

    def applied(ref, h, skip, count, c, low, grounds):
        at = pl.ds(c, TILE)
        west = pl.ds(c - 1, TILE)
        east = pl.ds(c + 1, TILE)
        column = c + lax.broadcasted_iota(jnp.int32, (TILE, LANES), 0)
        mid = ref[h, skip + 1, at, :]
        flow = V[low, at, :] * ref[h, skip, at, :]
        for k in range(count):
            after = ref[h, skip + k + 2, at, :]
            v = V[low + k + 1, at, :]
            grounded = column == grounds[k]
            diag = D[low + k, at, :]
            out = jnp.where(grounded, diag + 1.0, diag) * mid - flow
            out = out - v * after
            out = out - H[low + k, west, :] * ref[h, skip + 1 + k, west, :]
            out = out - H[low + k, at, :] * ref[h, skip + 1 + k, east, :]
            yield k, out, mid, grounded, column
            flow = v * mid
            mid = after

    def zeros():
        return tuple(jnp.zeros((TILE, LANES), jnp.float32) for _ in range(7))

    def compute(h, j, acc):
        def named(cells, top, count):
            return [shape_of(cells, h, top + k) for k in range(count)]

        count_r, count_w = 2 * rows, 2 * rows - 2
        src_r, gnd_r = named(source_ref, -2, count_r), named(ground_ref, -2, count_r)
        gnd_w = named(ground_ref, -1, count_w)
        src_u, gnd_u = named(source_ref, 0, rows), named(ground_ref, 0, rows)

        def pass_r(t, _):
            c = pl.multiple_of(t * TILE, TILE)
            for k, a, _mid, _g, column in applied(X, h, 1, count_r, c, 0, gnd_r):
                R[h, k, pl.ds(c, TILE), :] = jnp.where(column == src_r[k], 1.0 - a, -a)
            return 0

        def pass_w(t, _):
            c = pl.multiple_of(t * TILE, TILE)
            for k, a, _mid, _g, _column in applied(R, h, 0, count_w, c, 1, gnd_w):
                W[h, k, pl.ds(c, TILE), :] = a
            return 0

        def pass_u(t, acc):
            c = pl.multiple_of(t * TILE, TILE)
            at = pl.ds(c, TILE)
            to = pl.ds(c - PAD, TILE)
            for k, u, w, grounded, column in applied(W, h, 0, rows, c, 2, gnd_u):
                r = R[h, 2 + k, at, :]
                x = X[h, rows + k, at, :]
                if h < halves - 1:
                    U[h, k, to, :] = u
                else:
                    for place, value in enumerate((x, r, w, u)):
                        field_ref[place, k, to, :] = value
                sign = jnp.where(column == src_u[k], 1.0, 0.0) - jnp.where(grounded, 1.0, 0.0)
                terms = (r * r, r * w, w * w, w * u, sign * x, sign * r, sign * w)
                acc = tuple(s + term for s, term in zip(acc, terms))
            return acc

        def sweep(lag, step, carry):
            bounds = own_at[h]
            begin, end = (1, tiles - 1) if lag < 3 else (2, tiles - 2)
            offset = PAD // TILE - lag
            final = j == len(bounds) - 2
            start = begin if j == 0 else offset + core + bounds[j]
            count = (end - 1 if final else offset + bounds[j + 1]) - (begin if j == 0 else offset + bounds[j])
            extra = core if j == 0 else 1 - core if final else None
            pairs = count // 2

            def pair(i, carry):
                return step(start + 2 * i + 1, step(start + 2 * i, carry))

            carry = lax.fori_loop(0, pairs, pair, carry)
            if count % 2:
                carry = step(start + 2 * pairs, carry)
            if extra is not None and not (j == 0 and final):
                carry = lax.fori_loop(start + count, start + count + extra, step, carry)
            return carry

        sweep(1, pass_r, 0)
        sweep(2, pass_w, 0)
        return sweep(3, pass_u, acc)

    def sum_copy(h, d):
        return remote(S.at[h, me], S.at[h, me], sum_send.at[0], sum_recv.at[h], (me + d) % n)

    def send_sums(h, acc):
        sums = [jnp.sum(s, axis=0, keepdims=True) for s in acc]
        S[h, me] = jnp.concatenate(sums + [jnp.zeros((1, LANES), jnp.float32)], 0)
        lax.fori_loop(1, n, lambda d, _: (sum_copy(h, d).start(), 0)[1], 0)

    def totals(h):
        arrived(S.at[h, pl.ds(0, n - 1)], sum_recv.at[h])
        total = S[h, 0]
        for k in range(1, n):
            total = total + S[h, k]
        m0, m1, m2, m3, ex, er, ew = (total[k:k + 1] for k in range(7))
        a0 = m0 / m1
        next_norm = a0 * (a0 * m2 - m1)
        ratio = next_norm / m0
        curve = m1 - a0 * (2.0 * m2 - a0 * m3)
        a1 = next_norm / (curve - ratio * next_norm / a0)
        p = a0 + a1 * (1.0 + ratio)
        q = a1 * a0
        drop_ref[h:h + 1, :] = ex + p * er - q * ew
        return p, q

    def finish(h):
        p, q = totals(h)
        p1 = jnp.broadcast_to(p, (TILE, LANES))
        q1 = jnp.broadcast_to(q, (TILE, LANES))

        def last(t, _):
            c = pl.multiple_of(t * TILE, TILE)
            at = pl.ds(c + PAD, TILE)
            to = pl.ds(c, TILE)
            for k in range(rows):
                r = R[h, 2 + k, at, :]
                w = W[h, 1 + k, at, :]
                pot_ref[h, k, to, :] = X[h, rows + k, at, :] + p1 * r - q1 * w
                res_ref[h, k, to, :] = r - p1 * w + q1 * U[h, k, to, :]
            return 0

        lax.fori_loop(0, cols // TILE, last, 0)

    for h in range(halves):
        side_wait(h)
        cross_wait(h, 0)

        @pl.when(has_diagonal)
        def _():
            cross_wait(h, 1)

        acc = zeros()
        relayed = 0
        for k in range(len(own_weights[h])):
            while relayed < parts[h] and pass_at[h][relayed] < own_at[h][k + 1]:
                @pl.when(gets_relay)
                def _():
                    arrived(X.at[h, pl.ds(odd * 2 * rows + 1, rows - 2), span(pass_at[h], relayed), :],
                            relay_recv.at[pass_sem[h] + relayed])
                    arrived(X.at[h, far_row, span(pass_at[h], relayed), :],
                            far_recv.at[pass_sem[h] + relayed])
                relayed += 1

            arrived(X.at[h, (1 - odd) * 2 * rows + odd * (rows - 1), span(own_at[h], k), :],
                    near_recv.at[own_sem[h] + k])
            acc = compute(h, k, acc)
        send_sums(h, acc)
        if h < halves - 1:
            for j in range(parts[h + 1]):
                relay(h + 1, j)
                onward(h + 1, j)

    for h in range(halves - 1):
        finish(h)

    p, q = totals(halves - 1)
    coef_ref[...] = jnp.concatenate([p, q, jnp.zeros((TILE - 2, LANES), jnp.float32)], 0)

    drained(C.at[0], cond_send.at[0])

    @pl.when(has_above)
    def _():
        drained(C.at[0], cond_send.at[1])
        drained(C.at[0, :, pl.ds(0, LANES)], cond_send.at[3])

    @pl.when(has_below)
    def _():
        drained(C.at[0], cond_send.at[2])
        drained(C.at[0, :, pl.ds(0, LANES)], cond_send.at[4])

    drained(X.at[:, pl.ds(0, rows), pl.ds(0, TILE), :], side_send.at[0])
    drained(X.at[:, pl.ds(0, rows - 1), pl.ds(0, TILE), :], cross_send.at[0])
    drained(X.at[:, pl.ds(0, rows - 1), pl.ds(0, TILE), :], edge_send.at[0])
    drained(X.at[:, pl.ds(0, 1), pl.ds(0, cols - TILE), :], near_send.at[0])
    drained(X.at[:, pl.ds(0, rows - 2), pl.ds(0, cols - TILE), :], pass_send.at[0])

    @pl.when(has_diagonal)
    def _():
        drained(X.at[:, pl.ds(0, rows - 1), pl.ds(0, TILE), :], cross_send.at[1])
        drained(X.at[:, pl.ds(0, rows - 1), pl.ds(0, TILE), :], far_send.at[0])

    @pl.when(can_relay)
    def _():
        drained(X.at[:, pl.ds(0, rows - 2), pl.ds(0, cols - TILE), :], relay_send.at[0])

    @pl.when(gets_relay)
    def _():
        drained(X.at[:, pl.ds(0, 1), pl.ds(0, cols - TILE), :], third_send.at[0])

    for h, j in lends:
        @pl.when(can_relay & jnp.logical_not(detours(pairs - 1 - rank, h, j)))
        def _():
            drained(X.at[h, guest, span(pass_at[h], j), :], onward_send.at[pass_sem[h] + j])

        if can_detour(h, j):
            @pl.when(can_relay & detours(rank + 1, h, j))
            def _():
                drained(X.at[h, lent, span(pass_at[h], j), :], forward_send.at[pass_sem[h] + j])

    drained(S.at[:, pl.ds(0, n - 1)], sum_send.at[0])


def closing(pot_ref, res_ref, field_ref, coef_ref, drop_ref, pot_out, res_out, drop_out,
            P1, Q1, sem):
    rows, cols = field_ref.shape[1], field_ref.shape[2]
    before = pot_ref.shape[0]

    def put(ref, out, h, c, count, k):
        return pltpu.make_async_copy(
            ref.at[:, pl.ds(c, count), :],
            out.at[0, :, pl.ds(c, count), pl.ds(h * LANES, LANES)], sem.at[k])

    for h in range(before):
        put(pot_ref.at[h], pot_out, h, 0, cols, 0).start()
        put(res_ref.at[h], res_out, h, 0, cols, 1).start()
    drop = pltpu.make_async_copy(drop_ref, drop_out, sem.at[2])
    drop.start()

    p1 = jnp.broadcast_to(coef_ref[0:1, :], (TILE, LANES))
    q1 = jnp.broadcast_to(coef_ref[1:2, :], (TILE, LANES))
    pieces = 4
    step = cols // pieces

    def last(t, _):
        c = pl.multiple_of(t * TILE, TILE)
        at = pl.ds(c, TILE)
        for k in range(rows):
            x, r, w, u = (field_ref[place, k, at, :] for place in range(4))
            P1[k, at, :] = x + p1 * r - q1 * w
            Q1[k, at, :] = r - p1 * w + q1 * u
        return 0

    for piece in range(pieces):
        lax.fori_loop(piece * step // TILE, (piece + 1) * step // TILE, last, 0, unroll=2)
        put(P1, pot_out, before, piece * step, step, 0).start()
        put(Q1, res_out, before, piece * step, step, 1).start()

    for k, out in enumerate((pot_out, res_out)):
        pltpu.make_async_copy(out, out, sem.at[k]).wait()
    drop.wait()


def solution(mesh):
    n = mesh.shape["tile"]
    rounds = max(1, (n // 2 - 1).bit_length())

    def shards(habitat, table, source_cell, ground_cell, start_potential):
        _, rows, cols, rhs = start_potential.shape
        halves = rhs // LANES
        width = cols + 2 * PAD
        f32 = jnp.float32
        dma = pltpu.SemaphoreType.DMA
        field = jax.ShapeDtypeStruct(start_potential.shape, f32)
        part = jax.ShapeDtypeStruct((halves - 1, rows, cols, LANES), f32)
        drops = jax.ShapeDtypeStruct((halves, LANES), f32)
        vmem = pl.BlockSpec(memory_space=pltpu.VMEM)
        hbm = pl.BlockSpec(memory_space=pltpu.HBM)
        pass_weights = ((32, 31),) * (halves - 1) + ((13, 13, 13, 12, 12),)
        own_weights = ((32, 31),) * (halves - 1) + ((9, 9, 9, 9, 9, 8, 6, 4),)
        passes, owns = sum(map(len, pass_weights)), sum(map(len, own_weights))
        stages = pl.pallas_call(
            functools.partial(kernel, n, rows, cols, rounds, pass_weights, own_weights),
            out_shape=(part, part, jax.ShapeDtypeStruct((4, rows, cols, LANES), f32),
                       jax.ShapeDtypeStruct((TILE, LANES), f32), drops),
            in_specs=[hbm] * 5,
            out_specs=(vmem,) * 5,
            scratch_shapes=[
                pltpu.VMEM((halves, 3 * rows, width, LANES), f32),
                pltpu.VMEM((halves, 2 * rows, width, LANES), f32),
                pltpu.VMEM((halves, 2 * rows - 2, width, LANES), f32),
                pltpu.VMEM((halves - 1, rows, cols, LANES), f32),
                pltpu.VMEM((2 * rows + 1, width, LANES), f32),
                pltpu.VMEM((2 * rows, width, LANES), f32),
                pltpu.VMEM((2 * rows, width, LANES), f32),
                pltpu.VMEM((6, 2 * rows, cols), f32),
                pltpu.VMEM((width, LANES), f32),
                pltpu.VMEM((width, LANES), f32),
                pltpu.VMEM((width, LANES), f32),
                pltpu.VMEM((halves, n, TILE, LANES), f32),
                pltpu.SMEM(table.shape, f32),
                pltpu.VMEM(habitat.shape, jnp.int32),
                pltpu.VMEM((halves, LANES), jnp.int32),
                pltpu.VMEM((halves, LANES), jnp.int32),
                dma((4,)), dma((halves,)),
                dma((5,)), dma((halves,)), dma((halves, 2)), dma((halves, 2)),
                dma((passes,)), dma((passes,)), dma((passes,)), dma((passes,)), dma((passes,)), dma((owns,)),
                dma((halves,)), dma((5,)), dma((1,)), dma((2,)),
                dma((1,)), dma((1,)), dma((1,)), dma((1,)), dma((1,)), dma((1,)),
                dma((passes,)), dma((passes,)), dma((1,)),
                pltpu.SemaphoreType.REGULAR((rounds,)),
            ],
            compiler_params=pltpu.CompilerParams(
                collective_id=0, has_side_effects=True, vmem_limit_bytes=32 * 2**20),
        )(*(pltpu.with_memory_space_constraint(value, pltpu.HBM) for value in (
            table, habitat, source_cell.reshape(halves, LANES),
            ground_cell.reshape(halves, LANES), start_potential)))
        potentials, residual, drop = pl.pallas_call(
            closing,
            out_shape=(field, field, drops),
            in_specs=[vmem] * 5,
            out_specs=(hbm,) * 3,
            scratch_shapes=[
                pltpu.VMEM((rows, cols, LANES), f32),
                pltpu.VMEM((rows, cols, LANES), f32),
                dma((3,)),
            ],
            compiler_params=pltpu.CompilerParams(vmem_limit_bytes=16 * 2**20),
        )(*stages)
        return potentials, residual, drop.reshape(rhs)

    placed = (
        P(("grp", "tile"), None, None),
        P(),
        P("grp"),
        P("grp"),
        P(("grp", "tile"), None, None, None),
    )
    return jax.shard_map(
        shards,
        mesh=mesh,
        in_specs=placed,
        out_specs=(placed[4], placed[4], P("grp")),
        check_vma=False,
    )
```

```python
import functools

import jax
import jax.numpy as jnp
from jax import lax
from jax.experimental import pallas as pl
from jax.experimental.pallas import tpu as pltpu
from jax.sharding import PartitionSpec as P

LANES = 128
TILE = 8
PAD = 2 * TILE
MESH = pl.DeviceIdType.MESH


def cuts(total, weights):
    bounds, seen = [0], 0
    for weight in weights:
        seen += weight
        bounds.append(total * seen // sum(weights))
    return bounds


def kernel(n, rows, cols, rounds, pass_weights, own_weights,
           table_hbm, habitat_hbm, source_hbm, ground_hbm, start_ref,
           pot_ref, res_ref, field_ref, coef_ref, drop_ref,
           X, R, W, U, V, H, D, C, T, TV, TH, S,
           table_ref, habitat_ref, source_ref, ground_ref, small_sem, load_sem,
           cond_recv, side_recv, edge_recv, cross_recv, pass_recv, relay_recv, third_recv, help_recv, far_recv, near_recv,
           sum_recv, cond_send, side_send, cross_send, near_send, edge_send, far_send, relay_send, pass_send, third_send, onward_send, forward_send, sum_send, hello):
    halves = X.shape[0]
    width = cols + 2 * PAD
    me = lax.axis_index("tile")
    chips = n // 2
    chip = me // 2
    core = me % 2
    odd = chip % 2
    side = me + 1 - 2 * core
    partner = me + 2 - 4 * odd
    diagonal = me - 2 + 4 * odd
    relay_to = me + 4 - 8 * odd
    relay_from = me - 4 + 8 * odd
    has_above = chip > 0
    has_below = chip < chips - 1
    has_diagonal = jnp.where(odd == 0, chip > 0, chip < chips - 1)
    can_relay = jnp.where(odd == 0, chip + 2 < chips, chip >= 2)
    gets_relay = jnp.where(odd == 0, chip >= 2, chip + 2 < chips)
    own = pl.ds(PAD, cols)
    body = cols // TILE - 1
    pass_at = [cuts(body, weights) for weights in pass_weights]
    pass_sem = cuts(sum(map(len, pass_weights)), list(map(len, pass_weights)))
    own_sem = cuts(sum(map(len, own_weights)), list(map(len, own_weights)))
    own_at = [cuts(body, weights) for weights in own_weights]

    def remote(src, dst, send, recv, target):
        return pltpu.make_async_remote_copy(
            src_ref=src, dst_ref=dst, send_sem=send, recv_sem=recv,
            device_id={"tile": target}, device_id_type=MESH)

    def arrived(place, recv):
        remote(place, place, near_send.at[0], recv, partner).wait_recv()

    def drained(place, send):
        remote(place, place, send, sum_recv.at[0], partner).wait_send()

    def signal(sem, target):
        pl.semaphore_signal(sem, inc=1, device_id={"tile": target}, device_id_type=MESH)

    def load(h):
        return pltpu.make_async_copy(
            start_ref.at[0, :, :, pl.ds(h * LANES, LANES)], X.at[h, pl.ds(rows, rows), own, :],
            load_sem.at[h])

    smalls = [
        pltpu.make_async_copy(src, dst, small_sem.at[k])
        for k, (src, dst) in enumerate((
            (table_hbm, table_ref), (habitat_hbm, habitat_ref),
            (source_hbm, source_ref), (ground_hbm, ground_ref)))
    ]

    barrier = pltpu.get_barrier_semaphore()
    signal(barrier, side)

    @pl.when(has_above)
    def _():
        signal(barrier, me - 2)
        signal(barrier, side - 2)

    @pl.when(has_below)
    def _():
        signal(barrier, me + 2)
        signal(barrier, side + 2)

    @pl.when(gets_relay)
    def _():
        signal(barrier, relay_from)

    @pl.when(can_relay)
    def _():
        signal(barrier, relay_to)

    for h in range(halves):
        load(h).start()
    for copy in smalls:
        copy.start()

    inner = pl.multiple_of(PAD + (1 - core) * (cols - TILE), TILE)
    outer = pl.multiple_of((1 - core) * TILE + core * (PAD + cols), TILE)
    halo = pl.multiple_of(core * TILE + (1 - core) * (PAD + cols), TILE)
    inner_at, outer_at, halo_at = pl.ds(inner, TILE), pl.ds(outer, TILE), pl.ds(halo, TILE)

    def span(bounds, j):
        start = pl.multiple_of(PAD + core * TILE + bounds[j] * TILE, TILE)
        return pl.ds(start, (bounds[j + 1] - bounds[j]) * TILE)

    def side_copy(h):
        place = pl.ds(rows, rows)
        return remote(X.at[h, place, inner_at, :], X.at[h, place, outer_at, :],
                      side_send.at[0], side_recv.at[h], side)

    def side_wait(h):
        arrived(X.at[h, pl.ds(rows, rows), halo_at, :], side_recv.at[h])

    def edge_near(h):
        return remote(X.at[h, pl.ds(rows + 1 - odd, rows - 1), inner_at, :],
                      X.at[h, pl.ds(odd * 2 * rows + 1 - odd, rows - 1), inner_at, :],
                      edge_send.at[0], edge_recv.at[h, 0], partner)

    def edge_far(h):
        return remote(X.at[h, pl.ds(rows + odd, rows - 1), inner_at, :],
                      X.at[h, pl.ds((1 - odd) * 2 * rows + odd, rows - 1), inner_at, :],
                      far_send.at[0], edge_recv.at[h, 1], diagonal)

    near_rows = pl.ds((1 - odd) * 2 * rows + odd, rows - 1)
    far_rows = pl.ds(odd * 2 * rows + 1 - odd, rows - 1)

    def cross(h, k):
        place = (near_rows, far_rows)[k]
        return remote(X.at[h, place, inner_at, :], X.at[h, place, outer_at, :],
                      cross_send.at[k], cross_recv.at[h, k], side)

    def cross_wait(h, k):
        arrived(X.at[h, (near_rows, far_rows)[k], halo_at, :], cross_recv.at[h, k])

    rank = jnp.where(odd == 0, chip // 2, chips // 2 - 1 - chip // 2)
    pairs, tally = chips // 2, halves * body

    def detours(k, h, j):
        return (pairs - k) * 2 * tally > pairs * (2 * h * body + pass_at[h][j] + pass_at[h][j + 1])

    def can_detour(h, j):
        return pairs > 1 and detours(1, h, j)

    outward = rows + odd * (rows - 1)
    lent = odd * (3 * rows - 1)
    guest = (1 - odd) * (3 * rows - 1)
    far_row = odd * 2 * rows + (1 - odd) * (rows - 1)
    far_there = (1 - odd) * 2 * rows + odd * (rows - 1)

    def pass_copy(h, j):
        at = span(pass_at[h], j)
        return remote(X.at[h, pl.ds(rows + 1, rows - 2), at, :],
                      X.at[h, pl.ds(odd * 2 * rows + 1, rows - 2), at, :],
                      pass_send.at[0], pass_recv.at[pass_sem[h] + j], partner)

    def relay_copy(h, j):
        at = span(pass_at[h], j)
        return remote(X.at[h, pl.ds((1 - odd) * 2 * rows + 1, rows - 2), at, :],
                      X.at[h, pl.ds(odd * 2 * rows + 1, rows - 2), at, :],
                      relay_send.at[0], relay_recv.at[pass_sem[h] + j], relay_to)

    def third_copy(h, j):
        at = span(pass_at[h], j)
        return remote(X.at[h, outward, at, :], X.at[h, odd * (3 * rows - 1), at, :],
                      third_send.at[0], third_recv.at[pass_sem[h] + j], partner)

    def help_copy(h, j):
        at = span(pass_at[h], j)
        return remote(X.at[h, outward, at, :], X.at[h, lent, at, :],
                      third_send.at[0], help_recv.at[pass_sem[h] + j], relay_from)

    def onward_copy(h, j):
        at = span(pass_at[h], j)
        return remote(X.at[h, guest, at, :], X.at[h, far_row, at, :],
                      onward_send.at[pass_sem[h] + j], far_recv.at[pass_sem[h] + j], relay_to)

    def forward_copy(h, j):
        at = span(pass_at[h], j)
        return remote(X.at[h, lent, at, :], X.at[h, far_there, at, :],
                      forward_send.at[pass_sem[h] + j], far_recv.at[pass_sem[h] + j], partner)

    def near_copy(h, k):
        at = span(own_at[h], k)
        row = (1 - odd) * (rows - 1)
        return remote(X.at[h, rows + row, at, :], X.at[h, odd * 2 * rows + row, at, :],
                      near_send.at[0], near_recv.at[own_sem[h] + k], partner)

    for copy in smalls:
        copy.wait()
    cells = habitat_ref[0]
    cond = jnp.zeros(cells.shape, jnp.float32)
    for level in range(table_ref.shape[0]):
        cond = jnp.where(cells == level, table_ref[level], cond)
    C[5, 0:rows, :] = cond
    C[5, rows:2 * rows, :] = cond

    pl.semaphore_wait(
        barrier,
        1 + 2 * has_above.astype(jnp.int32) + 2 * has_below.astype(jnp.int32)
        + can_relay.astype(jnp.int32) + gets_relay.astype(jnp.int32))

    def cond_copy(target, slot, kind):
        return remote(C.at[5], C.at[slot], cond_send.at[kind], cond_recv.at[slot], target)

    def inner_lanes(which):
        return pl.ds(pl.multiple_of(which * (cols - LANES), LANES), LANES)

    def corner_copy(target, slot, kind):
        at = inner_lanes(1 - core)
        return remote(C.at[5, :, at], C.at[slot, :, at], cond_send.at[kind], cond_recv.at[slot], target)

    def corner_wait(slot):
        arrived(C.at[slot, :, inner_lanes(core)], cond_recv.at[slot])

    cond_copy(side, 2, 0).start()

    @pl.when(has_above)
    def _():
        cond_copy(me - 2, 1, 1).start()
        corner_copy(side - 2, 4, 3).start()

    @pl.when(has_below)
    def _():
        cond_copy(me + 2, 0, 2).start()
        corner_copy(side + 2, 3, 4).start()

    for h in range(halves):
        load(h).wait()
        side_copy(h).start()
        edge_near(h).start()

        @pl.when(has_diagonal)
        def _():
            edge_far(h).start()

    parts = list(map(len, pass_weights))

    for h in range(halves):
        for j in range(parts[h]):
            if can_detour(h, j):
                @pl.when(gets_relay & detours(rank, h, j))
                def _():
                    help_copy(h, j).start()

    def send_pass(h, j):
        pass_copy(h, j).start()

        @pl.when(gets_relay & jnp.logical_not(detours(rank, h, j)))
        def _():
            third_copy(h, j).start()

    send_pass(0, 0)

    def zero(ref, h, c):
        ref[h, :, c:c + TILE, :] = jnp.zeros((ref.shape[1], TILE, LANES), jnp.float32)

    for h in range(halves):
        for c in (0, width - TILE):
            zero(X, h, c)
            zero(R, h, c)
            zero(W, h, c)

        @pl.when(core == 0)
        def _():
            zero(X, h, TILE)

        @pl.when(core == 1)
        def _():
            zero(X, h, width - PAD)

        @pl.when(jnp.logical_not(has_above))
        def _():
            X[h, 1:rows] = jnp.zeros((rows - 1, width, LANES), jnp.float32)

        @pl.when(jnp.logical_not(has_below))
        def _():
            X[h, 2 * rows:3 * rows - 1] = jnp.zeros((rows - 1, width, LANES), jnp.float32)

    for h in range(halves):
        arrived(X.at[h, near_rows, inner_at, :], edge_recv.at[h, 0])
        cross(h, 0).start()

    @pl.when(has_diagonal)
    def _():
        for h in range(halves):
            arrived(X.at[h, far_rows, inner_at, :], edge_recv.at[h, 1])
            cross(h, 1).start()

    arrived(C.at[2], cond_recv.at[2])

    @pl.when(has_above)
    def _():
        arrived(C.at[0], cond_recv.at[0])
        corner_wait(3)

    @pl.when(has_below)
    def _():
        arrived(C.at[1], cond_recv.at[1])
        corner_wait(4)

    @pl.when(jnp.logical_not(has_above))
    def _():
        for slot in (0, 3):
            C[slot] = jnp.zeros(C.shape[1:], jnp.float32)

    @pl.when(jnp.logical_not(has_below))
    def _():
        for slot in (1, 4):
            C[slot] = jnp.zeros(C.shape[1:], jnp.float32)

    def greet(r):
        d = 2 << r

        @pl.when(me >= d)
        def _():
            signal(hello.at[r], me - d)

        @pl.when(me + d < n)
        def _():
            signal(hello.at[r], me + d)

    def greeted(r):
        d = 2 << r
        pl.semaphore_wait(hello.at[r], (me >= d).astype(jnp.int32) + (me + d < n).astype(jnp.int32))

    for j in range(1, parts[0]):
        send_pass(0, j)
    near_copy(0, 0).start()
    greet(0)

    first = lax.broadcasted_iota(jnp.int32, (2 * rows, LANES), 0) < rows

    def turned(above, here, below, j):
        lanes = slice(j * LANES, (j + 1) * LANES)
        top = jnp.where(first, C[above, :, lanes], C[here, :, lanes])
        blank = jnp.zeros((LANES - 4 * rows, LANES), jnp.float32)
        return jnp.transpose(jnp.concatenate([top, C[below, :, lanes], blank], 0))

    for j in range(cols // LANES):
        T[PAD + j * LANES:PAD + (j + 1) * LANES, :] = turned(0, 5, 1, j)
    for c in (0, TILE, width - PAD, width - TILE):
        T[c:c + TILE, :] = jnp.zeros((TILE, LANES), jnp.float32)

    @pl.when(core == 0)
    def _():
        T[width - PAD:width - TILE, :] = turned(3, 2, 4, 0)[0:TILE]

    @pl.when(core == 1)
    def _():
        T[TILE:PAD, :] = turned(3, 2, 4, cols // LANES - 1)[LANES - TILE:]

    def global_col(c):
        return core * cols - PAD + c + lax.broadcasted_iota(jnp.int32, (TILE, LANES), 0)

    global_row = chip * rows - rows + lax.broadcasted_iota(jnp.int32, (TILE, LANES), 1)
    total_rows, total_cols = chips * rows, 2 * cols

    def edges(t, _):
        c = pl.multiple_of(t * TILE, TILE)
        here = T[pl.ds(c, TILE), :]
        east = T[pl.ds(c + 1, TILE), :]
        south = pltpu.roll(here, LANES - 1, 1)
        gc = global_col(c)
        in_row = (global_row >= 0) & (global_row < total_rows - 1)
        TV[pl.ds(c, TILE), :] = jnp.where(in_row, 0.5 * (here + south), 0.0)
        in_col = (gc >= 0) & (gc < total_cols - 1)
        TH[pl.ds(c, TILE), :] = jnp.where(in_col, 0.5 * (here + east), 0.0)
        return 0

    TH[0:TILE, :] = jnp.zeros((TILE, LANES), jnp.float32)
    H[:, 0:TILE, :] = jnp.zeros((H.shape[0], TILE, LANES), jnp.float32)
    lax.fori_loop(1, width // TILE - 1, edges, 0, unroll=6)

    def spread(t, _):
        c = pl.multiple_of(t * TILE, TILE)
        at = pl.ds(c, TILE)
        v = TV[at, :]
        east = TH[at, :]
        west = TH[pl.ds(c - 1, TILE), :]
        diag = v + pltpu.roll(v, 1, 1) + east + west
        shape = (TILE, LANES)
        for k in range(2 * rows + 1):
            V[k, at, :] = jnp.broadcast_to(v[:, k + 1:k + 2], shape)
        for k in range(2 * rows):
            H[k, at, :] = jnp.broadcast_to(east[:, k + 2:k + 3], shape)
            D[k, at, :] = jnp.broadcast_to(diag[:, k + 2:k + 3], shape)
        return 0

    tiles = width // TILE

    def relay(h, j):
        arrived(X.at[h, pl.ds((1 - odd) * 2 * rows + 1, rows - 2), span(pass_at[h], j), :],
                pass_recv.at[pass_sem[h] + j])

        @pl.when(can_relay)
        def _():
            relay_copy(h, j).start()

    def onward(h, j):
        @pl.when(can_relay & jnp.logical_not(detours(pairs - 1 - rank, h, j)))
        def _():
            arrived(X.at[h, guest, span(pass_at[h], j), :], third_recv.at[pass_sem[h] + j])
            onward_copy(h, j).start()

    def forward(h, j):
        if can_detour(h, j):
            @pl.when(can_relay & detours(rank + 1, h, j))
            def _():
                arrived(X.at[h, lent, span(pass_at[h], j), :], help_recv.at[pass_sem[h] + j])
                forward_copy(h, j).start()

    def meet(r):
        if r < rounds:
            greeted(r)
            if r + 1 < rounds:
                greet(r + 1)

    steps = [[lambda j=j: relay(0, j), lambda j=j: onward(0, j)] for j in range(parts[0])]
    steps = sum(steps, [])
    lends = [(h, j) for h in range(halves) for j in range(parts[h])]
    splits = cuts(tiles - 2, [1] * len(steps))
    for i, step in enumerate(steps):
        lax.fori_loop(1 + splits[i], 1 + splits[i + 1], spread, 0)
        step()
        meet(i)
        if i == 0:
            for j in range(parts[0]):
                forward(0, j)
        if i == 1:
            for h, j in lends[parts[0]:]:
                forward(h, j)
            for h in range(1, halves):
                for j in range(parts[h]):
                    send_pass(h, j)
            for h in range(halves):
                for k in range(h == 0, len(own_weights[h])):
                    near_copy(h, k).start()
    for r in range(len(steps), rounds):
        meet(r)

    def shape_of(cells, h, top):
        base = (chip * rows + top) * total_cols + core * cols - PAD
        return jnp.broadcast_to(cells[h:h + 1, :] - base, (TILE, LANES))

    def applied(ref, h, skip, count, c, low, grounds):
        at = pl.ds(c, TILE)
        west = pl.ds(c - 1, TILE)
        east = pl.ds(c + 1, TILE)
        column = c + lax.broadcasted_iota(jnp.int32, (TILE, LANES), 0)
        mid = ref[h, skip + 1, at, :]
        flow = V[low, at, :] * ref[h, skip, at, :]
        for k in range(count):
            after = ref[h, skip + k + 2, at, :]
            v = V[low + k + 1, at, :]
            grounded = column == grounds[k]
            diag = D[low + k, at, :]
            out = jnp.where(grounded, diag + 1.0, diag) * mid - flow
            out = out - v * after
            out = out - H[low + k, west, :] * ref[h, skip + 1 + k, west, :]
            out = out - H[low + k, at, :] * ref[h, skip + 1 + k, east, :]
            yield k, out, mid, grounded, column
            flow = v * mid
            mid = after

    def zeros():
        return tuple(jnp.zeros((TILE, LANES), jnp.float32) for _ in range(7))

    def compute(h, j, acc):
        def named(cells, top, count):
            return [shape_of(cells, h, top + k) for k in range(count)]

        count_r, count_w = 2 * rows, 2 * rows - 2
        src_r, gnd_r = named(source_ref, -2, count_r), named(ground_ref, -2, count_r)
        gnd_w = named(ground_ref, -1, count_w)
        src_u, gnd_u = named(source_ref, 0, rows), named(ground_ref, 0, rows)

        def pass_r(t, _):
            c = pl.multiple_of(t * TILE, TILE)
            for k, a, _mid, _g, column in applied(X, h, 1, count_r, c, 0, gnd_r):
                R[h, k, pl.ds(c, TILE), :] = jnp.where(column == src_r[k], 1.0 - a, -a)
            return 0

        def pass_w(t, _):
            c = pl.multiple_of(t * TILE, TILE)
            for k, a, _mid, _g, _column in applied(R, h, 0, count_w, c, 1, gnd_w):
                W[h, k, pl.ds(c, TILE), :] = a
            return 0

        def pass_u(t, acc):
            c = pl.multiple_of(t * TILE, TILE)
            at = pl.ds(c, TILE)
            to = pl.ds(c - PAD, TILE)
            for k, u, w, grounded, column in applied(W, h, 0, rows, c, 2, gnd_u):
                r = R[h, 2 + k, at, :]
                x = X[h, rows + k, at, :]
                if h < halves - 1:
                    U[h, k, to, :] = u
                else:
                    for place, value in enumerate((x, r, w, u)):
                        field_ref[place, k, to, :] = value
                sign = jnp.where(column == src_u[k], 1.0, 0.0) - jnp.where(grounded, 1.0, 0.0)
                terms = (r * r, r * w, w * w, w * u, sign * x, sign * r, sign * w)
                acc = tuple(s + term for s, term in zip(acc, terms))
            return acc

        def sweep(lag, step, carry):
            bounds = own_at[h]
            begin, end = (1, tiles - 1) if lag < 3 else (2, tiles - 2)
            offset = PAD // TILE - lag
            final = j == len(bounds) - 2
            start = begin if j == 0 else offset + core + bounds[j]
            count = (end - 1 if final else offset + bounds[j + 1]) - (begin if j == 0 else offset + bounds[j])
            extra = core if j == 0 else 1 - core if final else None
            pairs = count // 2

            def pair(i, carry):
                return step(start + 2 * i + 1, step(start + 2 * i, carry))

            carry = lax.fori_loop(0, pairs, pair, carry)
            if count % 2:
                carry = step(start + 2 * pairs, carry)
            if extra is not None and not (j == 0 and final):
                carry = lax.fori_loop(start + count, start + count + extra, step, carry)
            return carry

        sweep(1, pass_r, 0)
        sweep(2, pass_w, 0)
        return sweep(3, pass_u, acc)

    def sum_copy(h, d):
        return remote(S.at[h, me], S.at[h, me], sum_send.at[0], sum_recv.at[h], (me + d) % n)

    def send_sums(h, acc):
        sums = [jnp.sum(s, axis=0, keepdims=True) for s in acc]
        S[h, me] = jnp.concatenate(sums + [jnp.zeros((1, LANES), jnp.float32)], 0)
        lax.fori_loop(1, n, lambda d, _: (sum_copy(h, d).start(), 0)[1], 0)

    def totals(h):
        arrived(S.at[h, pl.ds(0, n - 1)], sum_recv.at[h])
        total = S[h, 0]
        for k in range(1, n):
            total = total + S[h, k]
        m0, m1, m2, m3, ex, er, ew = (total[k:k + 1] for k in range(7))
        a0 = m0 / m1
        next_norm = a0 * (a0 * m2 - m1)
        ratio = next_norm / m0
        curve = m1 - a0 * (2.0 * m2 - a0 * m3)
        a1 = next_norm / (curve - ratio * next_norm / a0)
        p = a0 + a1 * (1.0 + ratio)
        q = a1 * a0
        drop_ref[h:h + 1, :] = ex + p * er - q * ew
        return p, q

    def finish(h):
        p, q = totals(h)
        p1 = jnp.broadcast_to(p, (TILE, LANES))
        q1 = jnp.broadcast_to(q, (TILE, LANES))

        def last(t, _):
            c = pl.multiple_of(t * TILE, TILE)
            at = pl.ds(c + PAD, TILE)
            to = pl.ds(c, TILE)
            for k in range(rows):
                r = R[h, 2 + k, at, :]
                w = W[h, 1 + k, at, :]
                pot_ref[h, k, to, :] = X[h, rows + k, at, :] + p1 * r - q1 * w
                res_ref[h, k, to, :] = r - p1 * w + q1 * U[h, k, to, :]
            return 0

        lax.fori_loop(0, cols // TILE, last, 0)

    for h in range(halves):
        side_wait(h)
        cross_wait(h, 0)

        @pl.when(has_diagonal)
        def _():
            cross_wait(h, 1)

    sums = [zeros() for _ in range(halves)]
    relayed = [0] * halves

    def advance(h, k):
        while relayed[h] < parts[h] and pass_at[h][relayed[h]] < own_at[h][k + 1]:
            j = relayed[h]

            @pl.when(gets_relay)
            def _():
                arrived(X.at[h, pl.ds(odd * 2 * rows + 1, rows - 2), span(pass_at[h], j), :],
                        relay_recv.at[pass_sem[h] + j])
                arrived(X.at[h, far_row, span(pass_at[h], j), :], far_recv.at[pass_sem[h] + j])
            relayed[h] += 1

        arrived(X.at[h, (1 - odd) * 2 * rows + odd * (rows - 1), span(own_at[h], k), :],
                near_recv.at[own_sem[h] + k])
        sums[h] = compute(h, k, sums[h])

    advance(0, 0)
    for h in range(1, halves):
        for j in range(parts[h]):
            relay(h, j)
            onward(h, j)
    for h in range(halves):
        for k in range(h == 0, len(own_weights[h])):
            advance(h, k)
        send_sums(h, sums[h])

    for h in range(halves - 1):
        finish(h)

    p, q = totals(halves - 1)
    coef_ref[...] = jnp.concatenate([p, q, jnp.zeros((TILE - 2, LANES), jnp.float32)], 0)

    drained(C.at[0], cond_send.at[0])

    @pl.when(has_above)
    def _():
        drained(C.at[0], cond_send.at[1])
        drained(C.at[0, :, pl.ds(0, LANES)], cond_send.at[3])

    @pl.when(has_below)
    def _():
        drained(C.at[0], cond_send.at[2])
        drained(C.at[0, :, pl.ds(0, LANES)], cond_send.at[4])

    drained(X.at[:, pl.ds(0, rows), pl.ds(0, TILE), :], side_send.at[0])
    drained(X.at[:, pl.ds(0, rows - 1), pl.ds(0, TILE), :], cross_send.at[0])
    drained(X.at[:, pl.ds(0, rows - 1), pl.ds(0, TILE), :], edge_send.at[0])
    drained(X.at[:, pl.ds(0, 1), pl.ds(0, cols - TILE), :], near_send.at[0])
    drained(X.at[:, pl.ds(0, rows - 2), pl.ds(0, cols - TILE), :], pass_send.at[0])

    @pl.when(has_diagonal)
    def _():
        drained(X.at[:, pl.ds(0, rows - 1), pl.ds(0, TILE), :], cross_send.at[1])
        drained(X.at[:, pl.ds(0, rows - 1), pl.ds(0, TILE), :], far_send.at[0])

    @pl.when(can_relay)
    def _():
        drained(X.at[:, pl.ds(0, rows - 2), pl.ds(0, cols - TILE), :], relay_send.at[0])

    @pl.when(gets_relay)
    def _():
        drained(X.at[:, pl.ds(0, 1), pl.ds(0, cols - TILE), :], third_send.at[0])

    for h, j in lends:
        @pl.when(can_relay & jnp.logical_not(detours(pairs - 1 - rank, h, j)))
        def _():
            drained(X.at[h, guest, span(pass_at[h], j), :], onward_send.at[pass_sem[h] + j])

        if can_detour(h, j):
            @pl.when(can_relay & detours(rank + 1, h, j))
            def _():
                drained(X.at[h, lent, span(pass_at[h], j), :], forward_send.at[pass_sem[h] + j])

    drained(S.at[:, pl.ds(0, n - 1)], sum_send.at[0])


def closing(pot_ref, res_ref, field_ref, coef_ref, drop_ref, pot_out, res_out, drop_out,
            P1, Q1, sem):
    rows, cols = field_ref.shape[1], field_ref.shape[2]
    before = pot_ref.shape[0]

    def put(ref, out, h, c, count, k):
        return pltpu.make_async_copy(
            ref.at[:, pl.ds(c, count), :],
            out.at[0, :, pl.ds(c, count), pl.ds(h * LANES, LANES)], sem.at[k])

    for h in range(before):
        put(pot_ref.at[h], pot_out, h, 0, cols, 0).start()
        put(res_ref.at[h], res_out, h, 0, cols, 1).start()
    drop = pltpu.make_async_copy(drop_ref, drop_out, sem.at[2])
    drop.start()

    p1 = jnp.broadcast_to(coef_ref[0:1, :], (TILE, LANES))
    q1 = jnp.broadcast_to(coef_ref[1:2, :], (TILE, LANES))
    pieces = 4
    step = cols // pieces

    def last(t, _):
        c = pl.multiple_of(t * TILE, TILE)
        at = pl.ds(c, TILE)
        for k in range(rows):
            x, r, w, u = (field_ref[place, k, at, :] for place in range(4))
            P1[k, at, :] = x + p1 * r - q1 * w
            Q1[k, at, :] = r - p1 * w + q1 * u
        return 0

    for piece in range(pieces):
        lax.fori_loop(piece * step // TILE, (piece + 1) * step // TILE, last, 0, unroll=2)
        put(P1, pot_out, before, piece * step, step, 0).start()
        put(Q1, res_out, before, piece * step, step, 1).start()

    for k, out in enumerate((pot_out, res_out)):
        pltpu.make_async_copy(out, out, sem.at[k]).wait()
    drop.wait()


def solution(mesh):
    n = mesh.shape["tile"]
    rounds = max(1, (n // 2 - 1).bit_length())

    def shards(habitat, table, source_cell, ground_cell, start_potential):
        _, rows, cols, rhs = start_potential.shape
        halves = rhs // LANES
        width = cols + 2 * PAD
        f32 = jnp.float32
        dma = pltpu.SemaphoreType.DMA
        field = jax.ShapeDtypeStruct(start_potential.shape, f32)
        part = jax.ShapeDtypeStruct((halves - 1, rows, cols, LANES), f32)
        drops = jax.ShapeDtypeStruct((halves, LANES), f32)
        vmem = pl.BlockSpec(memory_space=pltpu.VMEM)
        hbm = pl.BlockSpec(memory_space=pltpu.HBM)
        pass_weights = ((32, 31),) * (halves - 1) + ((14, 14, 14, 12, 9),)
        own_weights = ((48, 15),) * (halves - 1) + ((9, 9, 9, 9, 9, 8, 6, 4),)
        passes, owns = sum(map(len, pass_weights)), sum(map(len, own_weights))
        stages = pl.pallas_call(
            functools.partial(kernel, n, rows, cols, rounds, pass_weights, own_weights),
            out_shape=(part, part, jax.ShapeDtypeStruct((4, rows, cols, LANES), f32),
                       jax.ShapeDtypeStruct((TILE, LANES), f32), drops),
            in_specs=[hbm] * 5,
            out_specs=(vmem,) * 5,
            scratch_shapes=[
                pltpu.VMEM((halves, 3 * rows, width, LANES), f32),
                pltpu.VMEM((halves, 2 * rows, width, LANES), f32),
                pltpu.VMEM((halves, 2 * rows - 2, width, LANES), f32),
                pltpu.VMEM((halves - 1, rows, cols, LANES), f32),
                pltpu.VMEM((2 * rows + 1, width, LANES), f32),
                pltpu.VMEM((2 * rows, width, LANES), f32),
                pltpu.VMEM((2 * rows, width, LANES), f32),
                pltpu.VMEM((6, 2 * rows, cols), f32),
                pltpu.VMEM((width, LANES), f32),
                pltpu.VMEM((width, LANES), f32),
                pltpu.VMEM((width, LANES), f32),
                pltpu.VMEM((halves, n, TILE, LANES), f32),
                pltpu.SMEM(table.shape, f32),
                pltpu.VMEM(habitat.shape, jnp.int32),
                pltpu.VMEM((halves, LANES), jnp.int32),
                pltpu.VMEM((halves, LANES), jnp.int32),
                dma((4,)), dma((halves,)),
                dma((5,)), dma((halves,)), dma((halves, 2)), dma((halves, 2)),
                dma((passes,)), dma((passes,)), dma((passes,)), dma((passes,)), dma((passes,)), dma((owns,)),
                dma((halves,)), dma((5,)), dma((1,)), dma((2,)),
                dma((1,)), dma((1,)), dma((1,)), dma((1,)), dma((1,)), dma((1,)),
                dma((passes,)), dma((passes,)), dma((1,)),
                pltpu.SemaphoreType.REGULAR((rounds,)),
            ],
            compiler_params=pltpu.CompilerParams(
                collective_id=0, has_side_effects=True, vmem_limit_bytes=32 * 2**20),
        )(*(pltpu.with_memory_space_constraint(value, pltpu.HBM) for value in (
            table, habitat, source_cell.reshape(halves, LANES),
            ground_cell.reshape(halves, LANES), start_potential)))
        potentials, residual, drop = pl.pallas_call(
            closing,
            out_shape=(field, field, drops),
            in_specs=[vmem] * 5,
            out_specs=(hbm,) * 3,
            scratch_shapes=[
                pltpu.VMEM((rows, cols, LANES), f32),
                pltpu.VMEM((rows, cols, LANES), f32),
                dma((3,)),
            ],
            compiler_params=pltpu.CompilerParams(vmem_limit_bytes=16 * 2**20),
        )(*stages)
        return potentials, residual, drop.reshape(rhs)

    placed = (
        P(("grp", "tile"), None, None),
        P(),
        P("grp"),
        P("grp"),
        P(("grp", "tile"), None, None, None),
    )
    return jax.shard_map(
        shards,
        mesh=mesh,
        in_specs=placed,
        out_specs=(placed[4], placed[4], P("grp")),
        check_vma=False,
    )
```

```python
import functools

import jax
import jax.numpy as jnp
from jax import lax
from jax.experimental import pallas as pl
from jax.experimental.pallas import tpu as pltpu
from jax.sharding import PartitionSpec as P

LANES = 128
TILE = 8
PAD = 2 * TILE
MESH = pl.DeviceIdType.MESH


def cuts(total, weights):
    bounds, seen = [0], 0
    for weight in weights:
        seen += weight
        bounds.append(total * seen // sum(weights))
    return bounds


def kernel(n, rows, cols, rounds, pass_weights, own_weights,
           table_hbm, habitat_hbm, source_hbm, ground_hbm, start_ref,
           pot_ref, res_ref, field_ref, coef_ref, drop_ref,
           X, R, W, U, V, H, D, C, T, TV, TH, S,
           table_ref, habitat_ref, source_ref, ground_ref, small_sem, load_sem,
           cond_recv, side_recv, edge_recv, cross_recv, pass_recv, relay_recv, third_recv, help_recv, near_recv,
           sum_recv, cond_send, side_send, cross_send, near_send, edge_send, far_send, relay_send, pass_send, third_send, onward_send, forward_send, sum_send, hello):
    halves = X.shape[0]
    width = cols + 2 * PAD
    me = lax.axis_index("tile")
    chips = n // 2
    chip = me // 2
    core = me % 2
    odd = chip % 2
    side = me + 1 - 2 * core
    partner = me + 2 - 4 * odd
    diagonal = me - 2 + 4 * odd
    relay_to = me + 4 - 8 * odd
    relay_from = me - 4 + 8 * odd
    has_above = chip > 0
    has_below = chip < chips - 1
    has_diagonal = jnp.where(odd == 0, chip > 0, chip < chips - 1)
    can_relay = jnp.where(odd == 0, chip + 2 < chips, chip >= 2)
    gets_relay = jnp.where(odd == 0, chip >= 2, chip + 2 < chips)
    own = pl.ds(PAD, cols)
    body = cols // TILE - 1
    pass_at = [cuts(body, weights) for weights in pass_weights]
    pass_sem = cuts(sum(map(len, pass_weights)), list(map(len, pass_weights)))
    own_sem = cuts(sum(map(len, own_weights)), list(map(len, own_weights)))
    own_at = [cuts(body, weights) for weights in own_weights]

    def remote(src, dst, send, recv, target):
        return pltpu.make_async_remote_copy(
            src_ref=src, dst_ref=dst, send_sem=send, recv_sem=recv,
            device_id={"tile": target}, device_id_type=MESH)

    def arrived(place, recv):
        remote(place, place, near_send.at[0], recv, partner).wait_recv()

    def drained(place, send):
        remote(place, place, send, sum_recv.at[0], partner).wait_send()

    def signal(sem, target):
        pl.semaphore_signal(sem, inc=1, device_id={"tile": target}, device_id_type=MESH)

    def load(h):
        return pltpu.make_async_copy(
            start_ref.at[0, :, :, pl.ds(h * LANES, LANES)], X.at[h, pl.ds(rows, rows), own, :],
            load_sem.at[h])

    smalls = [
        pltpu.make_async_copy(src, dst, small_sem.at[k])
        for k, (src, dst) in enumerate((
            (table_hbm, table_ref), (habitat_hbm, habitat_ref),
            (source_hbm, source_ref), (ground_hbm, ground_ref)))
    ]

    for copy in smalls:
        copy.start()
    for h in range(halves):
        load(h).start()

    barrier = pltpu.get_barrier_semaphore()
    signal(barrier, side)

    @pl.when(has_above)
    def _():
        signal(barrier, me - 2)
        signal(barrier, side - 2)

    @pl.when(has_below)
    def _():
        signal(barrier, me + 2)
        signal(barrier, side + 2)

    @pl.when(gets_relay)
    def _():
        signal(barrier, relay_from)

    @pl.when(can_relay)
    def _():
        signal(barrier, relay_to)


    inner = pl.multiple_of(PAD + (1 - core) * (cols - TILE), TILE)
    outer = pl.multiple_of((1 - core) * TILE + core * (PAD + cols), TILE)
    halo = pl.multiple_of(core * TILE + (1 - core) * (PAD + cols), TILE)
    inner_at, outer_at, halo_at = pl.ds(inner, TILE), pl.ds(outer, TILE), pl.ds(halo, TILE)

    def span(bounds, j):
        start = pl.multiple_of(PAD + core * TILE + bounds[j] * TILE, TILE)
        return pl.ds(start, (bounds[j + 1] - bounds[j]) * TILE)

    def side_copy(h):
        place = pl.ds(rows, rows)
        return remote(X.at[h, place, inner_at, :], X.at[h, place, outer_at, :],
                      side_send.at[0], side_recv.at[h], side)

    def side_wait(h):
        arrived(X.at[h, pl.ds(rows, rows), halo_at, :], side_recv.at[h])

    def edge_near(h):
        return remote(X.at[h, pl.ds(rows + 1 - odd, rows - 1), inner_at, :],
                      X.at[h, pl.ds(odd * 2 * rows + 1 - odd, rows - 1), inner_at, :],
                      edge_send.at[0], edge_recv.at[h, 0], partner)

    def edge_far(h):
        return remote(X.at[h, pl.ds(rows + odd, rows - 1), inner_at, :],
                      X.at[h, pl.ds((1 - odd) * 2 * rows + odd, rows - 1), inner_at, :],
                      far_send.at[0], edge_recv.at[h, 1], diagonal)

    near_rows = pl.ds((1 - odd) * 2 * rows + odd, rows - 1)
    far_rows = pl.ds(odd * 2 * rows + 1 - odd, rows - 1)

    def cross(h, k):
        place = (near_rows, far_rows)[k]
        return remote(X.at[h, place, inner_at, :], X.at[h, place, outer_at, :],
                      cross_send.at[k], cross_recv.at[h, k], side)

    def cross_wait(h, k):
        arrived(X.at[h, (near_rows, far_rows)[k], halo_at, :], cross_recv.at[h, k])

    rank = jnp.where(odd == 0, chip // 2, chips // 2 - 1 - chip // 2)
    pairs, tally = chips // 2, halves * body

    def detours(k, h, j):
        return (pairs - k) * 2 * tally > pairs * (2 * h * body + pass_at[h][j] + pass_at[h][j + 1])

    def can_detour(h, j):
        return pairs > 1 and detours(1, h, j)

    outward = rows + odd * (rows - 1)
    lent = odd * (3 * rows - 1)
    guest = (1 - odd) * (3 * rows - 1)
    far_row = odd * 2 * rows + (1 - odd) * (rows - 1)
    far_there = (1 - odd) * 2 * rows + odd * (rows - 1)

    def pass_copy(h, j):
        at = span(pass_at[h], j)
        return remote(X.at[h, pl.ds(rows + 1, rows - 2), at, :],
                      X.at[h, pl.ds(odd * 2 * rows + 1, rows - 2), at, :],
                      pass_send.at[0], pass_recv.at[pass_sem[h] + j], partner)

    def relay_copy(h, j):
        at = span(pass_at[h], j)
        return remote(X.at[h, pl.ds((1 - odd) * 2 * rows + 1, rows - 2), at, :],
                      X.at[h, pl.ds(odd * 2 * rows + 1, rows - 2), at, :],
                      relay_send.at[0], relay_recv.at[pass_sem[h] + j], relay_to)

    def third_copy(h, j):
        at = span(pass_at[h], j)
        return remote(X.at[h, outward, at, :], X.at[h, odd * (3 * rows - 1), at, :],
                      third_send.at[0], third_recv.at[pass_sem[h] + j], partner)

    def help_copy(h, j):
        at = span(pass_at[h], j)
        return remote(X.at[h, outward, at, :], X.at[h, lent, at, :],
                      third_send.at[0], help_recv.at[pass_sem[h] + j], relay_from)

    def onward_copy(h, j):
        at = span(pass_at[h], j)
        return remote(X.at[h, guest, at, :], X.at[h, far_row, at, :],
                      onward_send.at[pass_sem[h] + j], relay_recv.at[pass_sem[h] + j], relay_to)

    def forward_copy(h, j):
        at = span(pass_at[h], j)
        return remote(X.at[h, lent, at, :], X.at[h, far_there, at, :],
                      forward_send.at[pass_sem[h] + j], relay_recv.at[pass_sem[h] + j], partner)

    def near_copy(h, k):
        at = span(own_at[h], k)
        row = (1 - odd) * (rows - 1)
        return remote(X.at[h, rows + row, at, :], X.at[h, odd * 2 * rows + row, at, :],
                      near_send.at[0], near_recv.at[own_sem[h] + k], partner)

    for copy in smalls:
        copy.wait()
    cells = habitat_ref[0]
    cond = jnp.zeros(cells.shape, jnp.float32)
    for level in range(table_ref.shape[0]):
        cond = jnp.where(cells == level, table_ref[level], cond)
    C[5, 0:rows, :] = cond
    C[5, rows:2 * rows, :] = cond

    pl.semaphore_wait(
        barrier,
        1 + 2 * has_above.astype(jnp.int32) + 2 * has_below.astype(jnp.int32)
        + can_relay.astype(jnp.int32) + gets_relay.astype(jnp.int32))

    def cond_copy(target, slot, kind):
        return remote(C.at[5], C.at[slot], cond_send.at[kind], cond_recv.at[slot], target)

    def inner_lanes(which):
        return pl.ds(pl.multiple_of(which * (cols - LANES), LANES), LANES)

    def corner_copy(target, slot, kind):
        at = inner_lanes(1 - core)
        return remote(C.at[5, :, at], C.at[slot, :, at], cond_send.at[kind], cond_recv.at[slot], target)

    def corner_wait(slot):
        arrived(C.at[slot, :, inner_lanes(core)], cond_recv.at[slot])

    cond_copy(side, 2, 0).start()

    @pl.when(has_above)
    def _():
        cond_copy(me - 2, 1, 1).start()
        corner_copy(side - 2, 4, 3).start()

    @pl.when(has_below)
    def _():
        cond_copy(me + 2, 0, 2).start()
        corner_copy(side + 2, 3, 4).start()

    for h in range(halves):
        load(h).wait()
        side_copy(h).start()
        edge_near(h).start()

        @pl.when(has_diagonal)
        def _():
            edge_far(h).start()

    parts = list(map(len, pass_weights))

    for h in range(halves):
        for j in range(parts[h]):
            if can_detour(h, j):
                @pl.when(gets_relay & detours(rank, h, j))
                def _():
                    help_copy(h, j).start()

    def send_pass(h, j):
        pass_copy(h, j).start()

        @pl.when(gets_relay & jnp.logical_not(detours(rank, h, j)))
        def _():
            third_copy(h, j).start()

    send_pass(0, 0)

    def zero(ref, h, c):
        ref[h, :, c:c + TILE, :] = jnp.zeros((ref.shape[1], TILE, LANES), jnp.float32)

    for h in range(halves):
        for c in (0, width - TILE):
            zero(X, h, c)
            zero(R, h, c)
            zero(W, h, c)

        @pl.when(core == 0)
        def _():
            zero(X, h, TILE)

        @pl.when(core == 1)
        def _():
            zero(X, h, width - PAD)

        @pl.when(jnp.logical_not(has_above))
        def _():
            X[h, 1:rows] = jnp.zeros((rows - 1, width, LANES), jnp.float32)

        @pl.when(jnp.logical_not(has_below))
        def _():
            X[h, 2 * rows:3 * rows - 1] = jnp.zeros((rows - 1, width, LANES), jnp.float32)

    for h in range(halves):
        arrived(X.at[h, near_rows, inner_at, :], edge_recv.at[h, 0])
        cross(h, 0).start()

    @pl.when(has_diagonal)
    def _():
        for h in range(halves):
            arrived(X.at[h, far_rows, inner_at, :], edge_recv.at[h, 1])
            cross(h, 1).start()

    arrived(C.at[2], cond_recv.at[2])

    @pl.when(has_above)
    def _():
        arrived(C.at[0], cond_recv.at[0])
        corner_wait(3)

    @pl.when(has_below)
    def _():
        arrived(C.at[1], cond_recv.at[1])
        corner_wait(4)

    @pl.when(jnp.logical_not(has_above))
    def _():
        for slot in (0, 3):
            C[slot] = jnp.zeros(C.shape[1:], jnp.float32)

    @pl.when(jnp.logical_not(has_below))
    def _():
        for slot in (1, 4):
            C[slot] = jnp.zeros(C.shape[1:], jnp.float32)

    def greet(r):
        d = 2 << r

        @pl.when(me >= d)
        def _():
            signal(hello.at[r], me - d)

        @pl.when(me + d < n)
        def _():
            signal(hello.at[r], me + d)

    def greeted(r):
        d = 2 << r
        pl.semaphore_wait(hello.at[r], (me >= d).astype(jnp.int32) + (me + d < n).astype(jnp.int32))

    for j in range(1, parts[0]):
        send_pass(0, j)
    early = len(own_weights[0]) - 1
    for k in range(early):
        near_copy(0, k).start()
    greet(0)

    first = lax.broadcasted_iota(jnp.int32, (2 * rows, LANES), 0) < rows

    def turned(above, here, below, j):
        lanes = slice(j * LANES, (j + 1) * LANES)
        top = jnp.where(first, C[above, :, lanes], C[here, :, lanes])
        blank = jnp.zeros((LANES - 4 * rows, LANES), jnp.float32)
        return jnp.transpose(jnp.concatenate([top, C[below, :, lanes], blank], 0))

    for j in range(cols // LANES):
        T[PAD + j * LANES:PAD + (j + 1) * LANES, :] = turned(0, 5, 1, j)
    for c in (0, TILE, width - PAD, width - TILE):
        T[c:c + TILE, :] = jnp.zeros((TILE, LANES), jnp.float32)

    @pl.when(core == 0)
    def _():
        T[width - PAD:width - TILE, :] = turned(3, 2, 4, 0)[0:TILE]

    @pl.when(core == 1)
    def _():
        T[TILE:PAD, :] = turned(3, 2, 4, cols // LANES - 1)[LANES - TILE:]

    def global_col(c):
        return core * cols - PAD + c + lax.broadcasted_iota(jnp.int32, (TILE, LANES), 0)

    global_row = chip * rows - rows + lax.broadcasted_iota(jnp.int32, (TILE, LANES), 1)
    total_rows, total_cols = chips * rows, 2 * cols

    def edges(t, _):
        c = pl.multiple_of(t * TILE, TILE)
        here = T[pl.ds(c, TILE), :]
        east = T[pl.ds(c + 1, TILE), :]
        south = pltpu.roll(here, LANES - 1, 1)
        gc = global_col(c)
        in_row = (global_row >= 0) & (global_row < total_rows - 1)
        TV[pl.ds(c, TILE), :] = jnp.where(in_row, 0.5 * (here + south), 0.0)
        in_col = (gc >= 0) & (gc < total_cols - 1)
        TH[pl.ds(c, TILE), :] = jnp.where(in_col, 0.5 * (here + east), 0.0)
        return 0

    TH[0:TILE, :] = jnp.zeros((TILE, LANES), jnp.float32)
    H[:, 0:TILE, :] = jnp.zeros((H.shape[0], TILE, LANES), jnp.float32)
    lax.fori_loop(1, width // TILE - 1, edges, 0, unroll=6)

    def spread(t, _):
        c = pl.multiple_of(t * TILE, TILE)
        at = pl.ds(c, TILE)
        v = TV[at, :]
        east = TH[at, :]
        west = TH[pl.ds(c - 1, TILE), :]
        diag = v + pltpu.roll(v, 1, 1) + east + west
        shape = (TILE, LANES)
        for k in range(2 * rows + 1):
            V[k, at, :] = jnp.broadcast_to(v[:, k + 1:k + 2], shape)
        for k in range(2 * rows):
            H[k, at, :] = jnp.broadcast_to(east[:, k + 2:k + 3], shape)
            D[k, at, :] = jnp.broadcast_to(diag[:, k + 2:k + 3], shape)
        return 0

    tiles = width // TILE

    def relay(h, j):
        arrived(X.at[h, pl.ds((1 - odd) * 2 * rows + 1, rows - 2), span(pass_at[h], j), :],
                pass_recv.at[pass_sem[h] + j])

        @pl.when(can_relay)
        def _():
            relay_copy(h, j).start()

    def onward(h, j):
        @pl.when(can_relay & jnp.logical_not(detours(pairs - 1 - rank, h, j)))
        def _():
            arrived(X.at[h, guest, span(pass_at[h], j), :], third_recv.at[pass_sem[h] + j])
            onward_copy(h, j).start()

    def forward(h, j):
        if can_detour(h, j):
            @pl.when(can_relay & detours(rank + 1, h, j))
            def _():
                arrived(X.at[h, lent, span(pass_at[h], j), :], help_recv.at[pass_sem[h] + j])
                forward_copy(h, j).start()

    def meet(r):
        if r < rounds:
            greeted(r)
            if r + 1 < rounds:
                greet(r + 1)

    steps = [[lambda j=j: relay(0, j), lambda j=j: onward(0, j)] for j in range(parts[0])]
    steps = sum(steps, [])
    lends = [(h, j) for h in range(halves) for j in range(parts[h])]
    splits = cuts(tiles - 2, [1] * len(steps))
    for i, step in enumerate(steps):
        lax.fori_loop(1 + splits[i], 1 + splits[i + 1], spread, 0)
        step()
        meet(i)
        if i == 0:
            for j in range(parts[0]):
                forward(0, j)
        if i == 1:
            for h, j in lends[parts[0]:]:
                forward(h, j)
            for h in range(1, halves):
                for j in range(parts[h]):
                    send_pass(h, j)
            for h in range(halves):
                for k in range(0 if h else early, len(own_weights[h])):
                    near_copy(h, k).start()
    for r in range(len(steps), rounds):
        meet(r)

    def shape_of(cells, h, top):
        base = (chip * rows + top) * total_cols + core * cols - PAD
        return jnp.broadcast_to(cells[h:h + 1, :] - base, (TILE, LANES))

    def applied(ref, h, skip, count, c, low, grounds):
        at = pl.ds(c, TILE)
        west = pl.ds(c - 1, TILE)
        east = pl.ds(c + 1, TILE)
        column = c + lax.broadcasted_iota(jnp.int32, (TILE, LANES), 0)
        mid = ref[h, skip + 1, at, :]
        flow = V[low, at, :] * ref[h, skip, at, :]
        for k in range(count):
            after = ref[h, skip + k + 2, at, :]
            v = V[low + k + 1, at, :]
            grounded = column == grounds[k]
            diag = D[low + k, at, :]
            out = jnp.where(grounded, diag + 1.0, diag) * mid - flow
            out = out - v * after
            out = out - H[low + k, west, :] * ref[h, skip + 1 + k, west, :]
            out = out - H[low + k, at, :] * ref[h, skip + 1 + k, east, :]
            yield k, out, mid, grounded, column
            flow = v * mid
            mid = after

    def zeros():
        return tuple(jnp.zeros((TILE, LANES), jnp.float32) for _ in range(10))

    def compute(h, j, acc):
        def named(cells, top, count):
            return [shape_of(cells, h, top + k) for k in range(count)]

        count_r, count_w = 2 * rows, 2 * rows - 2
        src_r, gnd_r = named(source_ref, -2, count_r), named(ground_ref, -2, count_r)
        gnd_w = named(ground_ref, -1, count_w)
        src_u, gnd_u = named(source_ref, 0, rows), named(ground_ref, 0, rows)

        def pass_r(t, _):
            c = pl.multiple_of(t * TILE, TILE)
            for k, a, _mid, _g, column in applied(X, h, 1, count_r, c, 0, gnd_r):
                R[h, k, pl.ds(c, TILE), :] = jnp.where(column == src_r[k], 1.0, 0.0) - a
            return 0

        def pass_w(t, _):
            c = pl.multiple_of(t * TILE, TILE)
            for k, a, _mid, _g, _column in applied(R, h, 0, count_w, c, 1, gnd_w):
                W[h, k, pl.ds(c, TILE), :] = a
            return 0

        def pass_u(t, acc):
            c = pl.multiple_of(t * TILE, TILE)
            at = pl.ds(c, TILE)
            to = pl.ds(c - PAD, TILE)
            for k, u, w, grounded, column in applied(W, h, 0, rows, c, 2, gnd_u):
                r = R[h, 2 + k, at, :]
                x = X[h, rows + k, at, :]
                if h < halves - 1:
                    U[h, k, to, :] = u
                else:
                    for place, value in enumerate((x, r, w, u)):
                        field_ref[place, k, to, :] = value
                terms = (r * r, r * w, w * w, w * u)
                sourced = column == src_u[k]
                acc = tuple(s + term for s, term in zip(acc, terms)) + tuple(
                    jnp.where(sourced, value, s) for s, value in zip(acc[4:7], (x, r, w))) + tuple(
                    jnp.where(grounded, value, s) for s, value in zip(acc[7:], (x, r, w)))
            return acc

        def sweep(lag, step, carry):
            bounds = own_at[h]
            begin, end = (1, tiles - 1) if lag < 3 else (2, tiles - 2)
            offset = PAD // TILE - lag
            final = j == len(bounds) - 2
            start = begin if j == 0 else offset + core + bounds[j]
            count = (end - 1 if final else offset + bounds[j + 1]) - (begin if j == 0 else offset + bounds[j])
            extra = core if j == 0 else 1 - core if final else None
            pairs = count // 2

            def pair(i, carry):
                return step(start + 2 * i + 1, step(start + 2 * i, carry))

            carry = lax.fori_loop(0, pairs, pair, carry)
            if count % 2:
                carry = step(start + 2 * pairs, carry)
            if extra is not None and not (j == 0 and final):
                carry = lax.fori_loop(start + count, start + count + extra, step, carry)
            return carry

        sweep(1, pass_r, 0)
        sweep(2, pass_w, 0)
        return sweep(3, pass_u, acc)

    def sum_copy(h, d):
        return remote(S.at[h, me], S.at[h, me], sum_send.at[0], sum_recv.at[h], (me + d) % n)

    def send_sums(h, acc):
        ends = tuple(at_source - at_ground for at_source, at_ground in zip(acc[4:7], acc[7:]))
        sums = [jnp.sum(s, axis=0, keepdims=True) for s in acc[:4] + ends]
        S[h, me] = jnp.concatenate(sums + [jnp.zeros((1, LANES), jnp.float32)], 0)
        lax.fori_loop(1, n, lambda d, _: (sum_copy(h, d).start(), 0)[1], 0)

    def totals(h):
        arrived(S.at[h, pl.ds(0, n - 1)], sum_recv.at[h])
        total = S[h, 0]
        for k in range(1, n):
            total = total + S[h, k]
        m0, m1, m2, m3, ex, er, ew = (total[k:k + 1] for k in range(7))
        a0 = m0 / m1
        next_norm = a0 * (a0 * m2 - m1)
        ratio = next_norm / m0
        curve = m1 - a0 * (2.0 * m2 - a0 * m3)
        a1 = next_norm / (curve - ratio * next_norm / a0)
        p = a0 + a1 * (1.0 + ratio)
        q = a1 * a0
        drop_ref[h:h + 1, :] = ex + p * er - q * ew
        return p, q

    def finish(h):
        p, q = totals(h)
        p1 = jnp.broadcast_to(p, (TILE, LANES))
        q1 = jnp.broadcast_to(q, (TILE, LANES))

        def last(t, _):
            c = pl.multiple_of(t * TILE, TILE)
            at = pl.ds(c + PAD, TILE)
            to = pl.ds(c, TILE)
            for k in range(rows):
                r = R[h, 2 + k, at, :]
                w = W[h, 1 + k, at, :]
                pot_ref[h, k, to, :] = X[h, rows + k, at, :] + p1 * r - q1 * w
                res_ref[h, k, to, :] = r - p1 * w + q1 * U[h, k, to, :]
            return 0

        lax.fori_loop(0, cols // TILE, last, 0)

    for h in range(halves):
        side_wait(h)
        cross_wait(h, 0)

        @pl.when(has_diagonal)
        def _():
            cross_wait(h, 1)

    sums = [zeros() for _ in range(halves)]
    relayed = [0] * halves

    def advance(h, k):
        while relayed[h] < parts[h] and pass_at[h][relayed[h]] < own_at[h][k + 1]:
            j = relayed[h]

            @pl.when(gets_relay)
            def _():
                arrived(X.at[h, far_rows, span(pass_at[h], j), :], relay_recv.at[pass_sem[h] + j])
            relayed[h] += 1

        arrived(X.at[h, (1 - odd) * 2 * rows + odd * (rows - 1), span(own_at[h], k), :],
                near_recv.at[own_sem[h] + k])
        sums[h] = compute(h, k, sums[h])

    for k in range(early):
        advance(0, k)
    for h in range(1, halves):
        for j in range(parts[h]):
            relay(h, j)
            onward(h, j)
    for h in range(halves):
        for k in range(0 if h else early, len(own_weights[h])):
            advance(h, k)
        send_sums(h, sums[h])

    for h in range(halves - 1):
        finish(h)

    p, q = totals(halves - 1)
    coef_ref[...] = jnp.concatenate([p, q, jnp.zeros((TILE - 2, LANES), jnp.float32)], 0)

    drained(C.at[0], cond_send.at[0])

    @pl.when(has_above)
    def _():
        drained(C.at[0], cond_send.at[1])
        drained(C.at[0, :, pl.ds(0, LANES)], cond_send.at[3])

    @pl.when(has_below)
    def _():
        drained(C.at[0], cond_send.at[2])
        drained(C.at[0, :, pl.ds(0, LANES)], cond_send.at[4])

    drained(X.at[:, pl.ds(0, rows), pl.ds(0, TILE), :], side_send.at[0])
    drained(X.at[:, pl.ds(0, rows - 1), pl.ds(0, TILE), :], cross_send.at[0])
    drained(X.at[:, pl.ds(0, rows - 1), pl.ds(0, TILE), :], edge_send.at[0])
    drained(X.at[:, pl.ds(0, 1), pl.ds(0, cols - TILE), :], near_send.at[0])
    drained(X.at[:, pl.ds(0, rows - 2), pl.ds(0, cols - TILE), :], pass_send.at[0])

    @pl.when(has_diagonal)
    def _():
        drained(X.at[:, pl.ds(0, rows - 1), pl.ds(0, TILE), :], cross_send.at[1])
        drained(X.at[:, pl.ds(0, rows - 1), pl.ds(0, TILE), :], far_send.at[0])

    @pl.when(can_relay)
    def _():
        drained(X.at[:, pl.ds(0, rows - 2), pl.ds(0, cols - TILE), :], relay_send.at[0])

    @pl.when(gets_relay)
    def _():
        drained(X.at[:, pl.ds(0, 1), pl.ds(0, cols - TILE), :], third_send.at[0])

    for h, j in lends:
        @pl.when(can_relay & jnp.logical_not(detours(pairs - 1 - rank, h, j)))
        def _():
            drained(X.at[h, guest, span(pass_at[h], j), :], onward_send.at[pass_sem[h] + j])

        if can_detour(h, j):
            @pl.when(can_relay & detours(rank + 1, h, j))
            def _():
                drained(X.at[h, lent, span(pass_at[h], j), :], forward_send.at[pass_sem[h] + j])

    drained(S.at[:, pl.ds(0, n - 1)], sum_send.at[0])


def closing(pot_ref, res_ref, field_ref, coef_ref, drop_ref, pot_out, res_out, drop_out,
            P1, Q1, sem):
    rows, cols = field_ref.shape[1], field_ref.shape[2]
    before = pot_ref.shape[0]

    def put(ref, out, h, c, count, k):
        return pltpu.make_async_copy(
            ref.at[:, pl.ds(c, count), :],
            out.at[0, :, pl.ds(c, count), pl.ds(h * LANES, LANES)], sem.at[k])

    for h in range(before):
        put(pot_ref.at[h], pot_out, h, 0, cols, 0).start()
        put(res_ref.at[h], res_out, h, 0, cols, 1).start()
    drop = pltpu.make_async_copy(drop_ref, drop_out, sem.at[2])
    drop.start()

    p1 = jnp.broadcast_to(coef_ref[0:1, :], (TILE, LANES))
    q1 = jnp.broadcast_to(coef_ref[1:2, :], (TILE, LANES))
    pieces = 4
    step = cols // pieces

    def last(t, _):
        c = pl.multiple_of(t * TILE, TILE)
        at = pl.ds(c, TILE)
        for k in range(rows):
            x, r, w, u = (field_ref[place, k, at, :] for place in range(4))
            P1[k, at, :] = x + p1 * r - q1 * w
            Q1[k, at, :] = r - p1 * w + q1 * u
        return 0

    for piece in range(pieces):
        lax.fori_loop(piece * step // TILE, (piece + 1) * step // TILE, last, 0, unroll=2)
        put(P1, pot_out, before, piece * step, step, 0).start()
        put(Q1, res_out, before, piece * step, step, 1).start()

    for k, out in enumerate((pot_out, res_out)):
        pltpu.make_async_copy(out, out, sem.at[k]).wait()
    drop.wait()


def solution(mesh):
    n = mesh.shape["tile"]
    rounds = max(1, (n // 2 - 1).bit_length())

    def shards(habitat, table, source_cell, ground_cell, start_potential):
        _, rows, cols, rhs = start_potential.shape
        halves = rhs // LANES
        width = cols + 2 * PAD
        f32 = jnp.float32
        dma = pltpu.SemaphoreType.DMA
        field = jax.ShapeDtypeStruct(start_potential.shape, f32)
        part = jax.ShapeDtypeStruct((halves - 1, rows, cols, LANES), f32)
        drops = jax.ShapeDtypeStruct((halves, LANES), f32)
        vmem = pl.BlockSpec(memory_space=pltpu.VMEM)
        hbm = pl.BlockSpec(memory_space=pltpu.HBM)
        pass_weights = ((32, 31),) * (halves - 1) + ((14, 14, 14, 12, 9),)
        own_weights = ((32, 20, 11),) * (halves - 1) + ((11, 11, 11, 11, 8, 7, 4),)
        passes, owns = sum(map(len, pass_weights)), sum(map(len, own_weights))
        stages = pl.pallas_call(
            functools.partial(kernel, n, rows, cols, rounds, pass_weights, own_weights),
            out_shape=(part, part, jax.ShapeDtypeStruct((4, rows, cols, LANES), f32),
                       jax.ShapeDtypeStruct((TILE, LANES), f32), drops),
            in_specs=[hbm] * 5,
            out_specs=(vmem,) * 5,
            scratch_shapes=[
                pltpu.VMEM((halves, 3 * rows, width, LANES), f32),
                pltpu.VMEM((halves, 2 * rows, width, LANES), f32),
                pltpu.VMEM((halves, 2 * rows - 2, width, LANES), f32),
                pltpu.VMEM((halves - 1, rows, cols, LANES), f32),
                pltpu.VMEM((2 * rows + 1, width, LANES), f32),
                pltpu.VMEM((2 * rows, width, LANES), f32),
                pltpu.VMEM((2 * rows, width, LANES), f32),
                pltpu.VMEM((6, 2 * rows, cols), f32),
                pltpu.VMEM((width, LANES), f32),
                pltpu.VMEM((width, LANES), f32),
                pltpu.VMEM((width, LANES), f32),
                pltpu.VMEM((halves, n, TILE, LANES), f32),
                pltpu.SMEM(table.shape, f32),
                pltpu.VMEM(habitat.shape, jnp.int32),
                pltpu.VMEM((halves, LANES), jnp.int32),
                pltpu.VMEM((halves, LANES), jnp.int32),
                dma((4,)), dma((halves,)),
                dma((5,)), dma((halves,)), dma((halves, 2)), dma((halves, 2)),
                dma((passes,)), dma((passes,)), dma((passes,)), dma((passes,)), dma((owns,)),
                dma((halves,)), dma((5,)), dma((1,)), dma((2,)),
                dma((1,)), dma((1,)), dma((1,)), dma((1,)), dma((1,)), dma((1,)),
                dma((passes,)), dma((passes,)), dma((1,)),
                pltpu.SemaphoreType.REGULAR((rounds,)),
            ],
            compiler_params=pltpu.CompilerParams(
                collective_id=0, has_side_effects=True, vmem_limit_bytes=32 * 2**20),
        )(*(pltpu.with_memory_space_constraint(value, pltpu.HBM) for value in (
            table, habitat, source_cell.reshape(halves, LANES),
            ground_cell.reshape(halves, LANES), start_potential)))
        potentials, residual, drop = pl.pallas_call(
            closing,
            out_shape=(field, field, drops),
            in_specs=[vmem] * 5,
            out_specs=(hbm,) * 3,
            scratch_shapes=[
                pltpu.VMEM((rows, cols, LANES), f32),
                pltpu.VMEM((rows, cols, LANES), f32),
                dma((3,)),
            ],
            compiler_params=pltpu.CompilerParams(vmem_limit_bytes=16 * 2**20),
        )(*stages)
        return potentials, residual, drop.reshape(rhs)

    placed = (
        P(("grp", "tile"), None, None),
        P(),
        P("grp"),
        P("grp"),
        P(("grp", "tile"), None, None, None),
    )
    return jax.shard_map(
        shards,
        mesh=mesh,
        in_specs=placed,
        out_specs=(placed[4], placed[4], P("grp")),
        check_vma=False,
    )
```

```python
import functools

import jax
import jax.numpy as jnp
from jax import lax
from jax.experimental import pallas as pl
from jax.experimental.pallas import tpu as pltpu
from jax.sharding import PartitionSpec as P

LANES = 128
TILE = 8
PAD = 2 * TILE
MESH = pl.DeviceIdType.MESH


def cuts(total, weights):
    bounds, seen = [0], 0
    for weight in weights:
        seen += weight
        bounds.append(total * seen // sum(weights))
    return bounds


def kernel(n, rows, cols, rounds, pass_weights, own_weights,
           table_hbm, habitat_hbm, source_hbm, ground_hbm, start_ref,
           pot_ref, res_ref, field_ref, coef_ref, drop_ref,
           X, R, W, U, V, H, D, C, T, TV, TH, S,
           table_ref, habitat_ref, source_ref, ground_ref, small_sem, load_sem,
           cond_recv, side_recv, edge_recv, cross_recv, pass_recv, relay_recv, third_recv, help_recv, near_recv,
           sum_recv, cond_send, side_send, cross_send, near_send, edge_send, far_send, relay_send, pass_send, third_send, onward_send, forward_send, sum_send, hello):
    halves = X.shape[0]
    width = cols + 2 * PAD
    me = lax.axis_index("tile")
    chips = n // 2
    chip = me // 2
    core = me % 2
    odd = chip % 2
    side = me + 1 - 2 * core
    partner = me + 2 - 4 * odd
    diagonal = me - 2 + 4 * odd
    relay_to = me + 4 - 8 * odd
    relay_from = me - 4 + 8 * odd
    has_above = chip > 0
    has_below = chip < chips - 1
    has_diagonal = jnp.where(odd == 0, chip > 0, chip < chips - 1)
    can_relay = jnp.where(odd == 0, chip + 2 < chips, chip >= 2)
    gets_relay = jnp.where(odd == 0, chip >= 2, chip + 2 < chips)
    own = pl.ds(PAD, cols)
    body = cols // TILE - 1
    pass_at = [cuts(body, weights) for weights in pass_weights]
    pass_sem = cuts(sum(map(len, pass_weights)), list(map(len, pass_weights)))
    own_sem = cuts(sum(map(len, own_weights)), list(map(len, own_weights)))
    own_at = [cuts(body, weights) for weights in own_weights]

    def remote(src, dst, send, recv, target):
        return pltpu.make_async_remote_copy(
            src_ref=src, dst_ref=dst, send_sem=send, recv_sem=recv,
            device_id={"tile": target}, device_id_type=MESH)

    def arrived(place, recv):
        remote(place, place, near_send.at[0], recv, partner).wait_recv()

    def drained(place, send):
        remote(place, place, send, sum_recv.at[0], partner).wait_send()

    def signal(sem, target):
        pl.semaphore_signal(sem, inc=1, device_id={"tile": target}, device_id_type=MESH)

    def load(h):
        return pltpu.make_async_copy(
            start_ref.at[0, :, :, pl.ds(h * LANES, LANES)], X.at[h, pl.ds(rows, rows), own, :],
            load_sem.at[h])

    smalls = [
        pltpu.make_async_copy(src, dst, small_sem.at[k])
        for k, (src, dst) in enumerate((
            (table_hbm, table_ref), (habitat_hbm, habitat_ref),
            (source_hbm, source_ref), (ground_hbm, ground_ref)))
    ]

    for copy in smalls:
        copy.start()
    for h in range(halves):
        load(h).start()

    barrier = pltpu.get_barrier_semaphore()
    signal(barrier, side)

    @pl.when(has_above)
    def _():
        signal(barrier, me - 2)
        signal(barrier, side - 2)

    @pl.when(has_below)
    def _():
        signal(barrier, me + 2)
        signal(barrier, side + 2)

    @pl.when(gets_relay)
    def _():
        signal(barrier, relay_from)

    @pl.when(can_relay)
    def _():
        signal(barrier, relay_to)


    inner = pl.multiple_of(PAD + (1 - core) * (cols - TILE), TILE)
    outer = pl.multiple_of((1 - core) * TILE + core * (PAD + cols), TILE)
    halo = pl.multiple_of(core * TILE + (1 - core) * (PAD + cols), TILE)
    inner_at, outer_at, halo_at = pl.ds(inner, TILE), pl.ds(outer, TILE), pl.ds(halo, TILE)

    def span(bounds, j):
        start = pl.multiple_of(PAD + core * TILE + bounds[j] * TILE, TILE)
        return pl.ds(start, (bounds[j + 1] - bounds[j]) * TILE)

    def side_copy(h):
        place = pl.ds(rows, rows)
        return remote(X.at[h, place, inner_at, :], X.at[h, place, outer_at, :],
                      side_send.at[0], side_recv.at[h], side)

    def side_wait(h):
        arrived(X.at[h, pl.ds(rows, rows), halo_at, :], side_recv.at[h])

    def edge_near(h):
        return remote(X.at[h, pl.ds(rows + 1 - odd, rows - 1), inner_at, :],
                      X.at[h, pl.ds(odd * 2 * rows + 1 - odd, rows - 1), inner_at, :],
                      edge_send.at[0], edge_recv.at[h, 0], partner)

    def edge_far(h):
        return remote(X.at[h, pl.ds(rows + odd, rows - 1), inner_at, :],
                      X.at[h, pl.ds((1 - odd) * 2 * rows + odd, rows - 1), inner_at, :],
                      far_send.at[0], edge_recv.at[h, 1], diagonal)

    near_rows = pl.ds((1 - odd) * 2 * rows + odd, rows - 1)
    far_rows = pl.ds(odd * 2 * rows + 1 - odd, rows - 1)

    def cross(h, k):
        place = (near_rows, far_rows)[k]
        return remote(X.at[h, place, inner_at, :], X.at[h, place, outer_at, :],
                      cross_send.at[k], cross_recv.at[h, k], side)

    def cross_wait(h, k):
        arrived(X.at[h, (near_rows, far_rows)[k], halo_at, :], cross_recv.at[h, k])

    rank = jnp.where(odd == 0, chip // 2, chips // 2 - 1 - chip // 2)
    pairs, tally = chips // 2, halves * body

    def detours(k, h, j):
        return (pairs - k) * 2 * tally > pairs * (2 * h * body + pass_at[h][j] + pass_at[h][j + 1])

    def can_detour(h, j):
        return pairs > 1 and detours(1, h, j)

    outward = rows + odd * (rows - 1)
    lent = odd * (3 * rows - 1)
    guest = (1 - odd) * (3 * rows - 1)
    far_row = odd * 2 * rows + (1 - odd) * (rows - 1)
    far_there = (1 - odd) * 2 * rows + odd * (rows - 1)

    def pass_copy(h, j):
        at = span(pass_at[h], j)
        return remote(X.at[h, pl.ds(rows + 1, rows - 2), at, :],
                      X.at[h, pl.ds(odd * 2 * rows + 1, rows - 2), at, :],
                      pass_send.at[0], pass_recv.at[pass_sem[h] + j], partner)

    def relay_copy(h, j):
        at = span(pass_at[h], j)
        return remote(X.at[h, pl.ds((1 - odd) * 2 * rows + 1, rows - 2), at, :],
                      X.at[h, pl.ds(odd * 2 * rows + 1, rows - 2), at, :],
                      relay_send.at[0], relay_recv.at[pass_sem[h] + j], relay_to)

    def third_copy(h, j):
        at = span(pass_at[h], j)
        return remote(X.at[h, outward, at, :], X.at[h, odd * (3 * rows - 1), at, :],
                      third_send.at[0], third_recv.at[pass_sem[h] + j], partner)

    def help_copy(h, j):
        at = span(pass_at[h], j)
        return remote(X.at[h, outward, at, :], X.at[h, lent, at, :],
                      third_send.at[0], help_recv.at[pass_sem[h] + j], relay_from)

    def onward_copy(h, j):
        at = span(pass_at[h], j)
        return remote(X.at[h, guest, at, :], X.at[h, far_row, at, :],
                      onward_send.at[pass_sem[h] + j], relay_recv.at[pass_sem[h] + j], relay_to)

    def forward_copy(h, j):
        at = span(pass_at[h], j)
        return remote(X.at[h, lent, at, :], X.at[h, far_there, at, :],
                      forward_send.at[pass_sem[h] + j], relay_recv.at[pass_sem[h] + j], partner)

    def near_copy(h, k):
        at = span(own_at[h], k)
        row = (1 - odd) * (rows - 1)
        return remote(X.at[h, rows + row, at, :], X.at[h, odd * 2 * rows + row, at, :],
                      near_send.at[0], near_recv.at[own_sem[h] + k], partner)

    for copy in smalls:
        copy.wait()
    cells = habitat_ref[0]
    cond = jnp.zeros(cells.shape, jnp.float32)
    for level in range(table_ref.shape[0]):
        cond = jnp.where(cells == level, table_ref[level], cond)
    C[5, 0:rows, :] = cond
    C[5, rows:2 * rows, :] = cond
    for slot in (0, 1):
        C[slot, rows:2 * rows, :] = jnp.zeros_like(cond)

    pl.semaphore_wait(
        barrier,
        1 + 2 * has_above.astype(jnp.int32) + 2 * has_below.astype(jnp.int32)
        + can_relay.astype(jnp.int32) + gets_relay.astype(jnp.int32))

    def cond_copy(target, slot, kind):
        return remote(C.at[5], C.at[slot], cond_send.at[kind], cond_recv.at[slot], target)

    def rows_copy(target, slot, kind):
        return remote(C.at[5, pl.ds(0, rows), :], C.at[slot, pl.ds(0, rows), :],
                      cond_send.at[kind], cond_recv.at[slot], target)

    def inner_lanes(which):
        return pl.ds(pl.multiple_of(which * (cols - LANES), LANES), LANES)

    def corner_copy(target, slot, kind):
        at = inner_lanes(1 - core)
        return remote(C.at[5, :, at], C.at[slot, :, at], cond_send.at[kind], cond_recv.at[slot], target)

    def corner_wait(slot):
        arrived(C.at[slot, :, inner_lanes(core)], cond_recv.at[slot])

    cond_copy(side, 2, 0).start()

    @pl.when(has_above)
    def _():
        rows_copy(me - 2, 1, 1).start()
        corner_copy(side - 2, 4, 3).start()

    @pl.when(has_below)
    def _():
        rows_copy(me + 2, 0, 2).start()
        corner_copy(side + 2, 3, 4).start()

    for h in range(halves):
        load(h).wait()
        side_copy(h).start()
        edge_near(h).start()

        @pl.when(has_diagonal)
        def _():
            edge_far(h).start()

    parts = list(map(len, pass_weights))

    for h in range(halves):
        for j in range(parts[h]):
            if can_detour(h, j):
                @pl.when(gets_relay & detours(rank, h, j))
                def _():
                    help_copy(h, j).start()

    def send_pass(h, j):
        pass_copy(h, j).start()

        @pl.when(gets_relay & jnp.logical_not(detours(rank, h, j)))
        def _():
            third_copy(h, j).start()

    send_pass(0, 0)

    def zero(ref, h, c):
        ref[h, :, c:c + TILE, :] = jnp.zeros((ref.shape[1], TILE, LANES), jnp.float32)

    for h in range(halves):
        for c in (0, width - TILE):
            zero(X, h, c)
            zero(R, h, c)
            zero(W, h, c)

        @pl.when(core == 0)
        def _():
            zero(X, h, TILE)

        @pl.when(core == 1)
        def _():
            zero(X, h, width - PAD)

        @pl.when(jnp.logical_not(has_above))
        def _():
            X[h, 1:rows] = jnp.zeros((rows - 1, width, LANES), jnp.float32)

        @pl.when(jnp.logical_not(has_below))
        def _():
            X[h, 2 * rows:3 * rows - 1] = jnp.zeros((rows - 1, width, LANES), jnp.float32)

    for h in range(halves):
        arrived(X.at[h, near_rows, inner_at, :], edge_recv.at[h, 0])
        cross(h, 0).start()

    @pl.when(has_diagonal)
    def _():
        for h in range(halves):
            arrived(X.at[h, far_rows, inner_at, :], edge_recv.at[h, 1])
            cross(h, 1).start()

    arrived(C.at[2], cond_recv.at[2])

    @pl.when(has_above)
    def _():
        arrived(C.at[0, pl.ds(0, rows), :], cond_recv.at[0])
        corner_wait(3)

    @pl.when(has_below)
    def _():
        arrived(C.at[1, pl.ds(0, rows), :], cond_recv.at[1])
        corner_wait(4)

    @pl.when(jnp.logical_not(has_above))
    def _():
        for slot in (0, 3):
            C[slot] = jnp.zeros(C.shape[1:], jnp.float32)

    @pl.when(jnp.logical_not(has_below))
    def _():
        for slot in (1, 4):
            C[slot] = jnp.zeros(C.shape[1:], jnp.float32)

    def greet(r):
        d = 2 << r

        @pl.when(me >= d)
        def _():
            signal(hello.at[r], me - d)

        @pl.when(me + d < n)
        def _():
            signal(hello.at[r], me + d)

    def greeted(r):
        d = 2 << r
        pl.semaphore_wait(hello.at[r], (me >= d).astype(jnp.int32) + (me + d < n).astype(jnp.int32))

    for j in range(1, parts[0]):
        send_pass(0, j)
    early = len(own_weights[0]) - 1
    for k in range(early):
        near_copy(0, k).start()
    greet(0)

    first = lax.broadcasted_iota(jnp.int32, (2 * rows, LANES), 0) < rows

    def turned(above, here, below, j):
        lanes = slice(j * LANES, (j + 1) * LANES)
        top = jnp.where(first, C[above, :, lanes], C[here, :, lanes])
        blank = jnp.zeros((LANES - 4 * rows, LANES), jnp.float32)
        return jnp.transpose(jnp.concatenate([top, C[below, :, lanes], blank], 0))

    for j in range(cols // LANES):
        T[PAD + j * LANES:PAD + (j + 1) * LANES, :] = turned(0, 5, 1, j)
    for c in (0, TILE, width - PAD, width - TILE):
        T[c:c + TILE, :] = jnp.zeros((TILE, LANES), jnp.float32)

    @pl.when(core == 0)
    def _():
        T[width - PAD:width - TILE, :] = turned(3, 2, 4, 0)[0:TILE]

    @pl.when(core == 1)
    def _():
        T[TILE:PAD, :] = turned(3, 2, 4, cols // LANES - 1)[LANES - TILE:]

    def global_col(c):
        return core * cols - PAD + c + lax.broadcasted_iota(jnp.int32, (TILE, LANES), 0)

    global_row = chip * rows - rows + lax.broadcasted_iota(jnp.int32, (TILE, LANES), 1)
    total_rows, total_cols = chips * rows, 2 * cols

    def edges(t, _):
        c = pl.multiple_of(t * TILE, TILE)
        here = T[pl.ds(c, TILE), :]
        east = T[pl.ds(c + 1, TILE), :]
        south = pltpu.roll(here, LANES - 1, 1)
        gc = global_col(c)
        in_row = (global_row >= 0) & (global_row < total_rows - 1)
        TV[pl.ds(c, TILE), :] = jnp.where(in_row, 0.5 * (here + south), 0.0)
        in_col = (gc >= 0) & (gc < total_cols - 1)
        TH[pl.ds(c, TILE), :] = jnp.where(in_col, 0.5 * (here + east), 0.0)
        return 0

    TH[0:TILE, :] = jnp.zeros((TILE, LANES), jnp.float32)
    H[:, 0:TILE, :] = jnp.zeros((H.shape[0], TILE, LANES), jnp.float32)
    lax.fori_loop(1, width // TILE - 1, edges, 0, unroll=6)

    def spread(t, _):
        c = pl.multiple_of(t * TILE, TILE)
        at = pl.ds(c, TILE)
        v = TV[at, :]
        east = TH[at, :]
        west = TH[pl.ds(c - 1, TILE), :]
        diag = v + pltpu.roll(v, 1, 1) + east + west
        shape = (TILE, LANES)
        for k in range(2 * rows + 1):
            V[k, at, :] = jnp.broadcast_to(v[:, k + 1:k + 2], shape)
        for k in range(2 * rows):
            H[k, at, :] = jnp.broadcast_to(east[:, k + 2:k + 3], shape)
            D[k, at, :] = jnp.broadcast_to(diag[:, k + 2:k + 3], shape)
        return 0

    tiles = width // TILE

    def relay(h, j):
        arrived(X.at[h, pl.ds((1 - odd) * 2 * rows + 1, rows - 2), span(pass_at[h], j), :],
                pass_recv.at[pass_sem[h] + j])

        @pl.when(can_relay)
        def _():
            relay_copy(h, j).start()

    def onward(h, j):
        @pl.when(can_relay & jnp.logical_not(detours(pairs - 1 - rank, h, j)))
        def _():
            arrived(X.at[h, guest, span(pass_at[h], j), :], third_recv.at[pass_sem[h] + j])
            onward_copy(h, j).start()

    def forward(h, j):
        if can_detour(h, j):
            @pl.when(can_relay & detours(rank + 1, h, j))
            def _():
                arrived(X.at[h, lent, span(pass_at[h], j), :], help_recv.at[pass_sem[h] + j])
                forward_copy(h, j).start()

    def meet(r):
        if r < rounds:
            greeted(r)
            if r + 1 < rounds:
                greet(r + 1)

    steps = [[lambda j=j: relay(0, j), lambda j=j: onward(0, j)] for j in range(parts[0])]
    steps = sum(steps, [])
    lends = [(h, j) for h in range(halves) for j in range(parts[h])]
    splits = cuts(tiles - 2, [1] * len(steps))
    for i, step in enumerate(steps):
        lax.fori_loop(1 + splits[i], 1 + splits[i + 1], spread, 0)
        step()
        meet(i)
        if i == 0:
            for j in range(parts[0]):
                forward(0, j)
        if i == 1:
            for h, j in lends[parts[0]:]:
                forward(h, j)
            for h in range(1, halves):
                for j in range(parts[h]):
                    send_pass(h, j)
            for h in range(halves):
                for k in range(0 if h else early, len(own_weights[h])):
                    near_copy(h, k).start()
    for r in range(len(steps), rounds):
        meet(r)

    def shape_of(cells, h, top):
        base = (chip * rows + top) * total_cols + core * cols - PAD
        return jnp.broadcast_to(cells[h:h + 1, :] - base, (TILE, LANES))

    def applied(ref, h, skip, count, c, low, grounds):
        at = pl.ds(c, TILE)
        west = pl.ds(c - 1, TILE)
        east = pl.ds(c + 1, TILE)
        column = c + lax.broadcasted_iota(jnp.int32, (TILE, LANES), 0)
        mid = ref[h, skip + 1, at, :]
        flow = V[low, at, :] * ref[h, skip, at, :]
        for k in range(count):
            after = ref[h, skip + k + 2, at, :]
            v = V[low + k + 1, at, :]
            grounded = column == grounds[k]
            diag = D[low + k, at, :]
            out = jnp.where(grounded, diag + 1.0, diag) * mid - flow
            out = out - v * after
            out = out - H[low + k, west, :] * ref[h, skip + 1 + k, west, :]
            out = out - H[low + k, at, :] * ref[h, skip + 1 + k, east, :]
            yield k, out, mid, grounded, column
            flow = v * mid
            mid = after

    def zeros():
        return tuple(jnp.zeros((TILE, LANES), jnp.float32) for _ in range(10))

    def compute(h, j, acc):
        def named(cells, top, count):
            return [shape_of(cells, h, top + k) for k in range(count)]

        count_r, count_w = 2 * rows, 2 * rows - 2
        src_r, gnd_r = named(source_ref, -2, count_r), named(ground_ref, -2, count_r)
        gnd_w = named(ground_ref, -1, count_w)
        src_u, gnd_u = named(source_ref, 0, rows), named(ground_ref, 0, rows)

        def pass_r(t, _):
            c = pl.multiple_of(t * TILE, TILE)
            for k, a, _mid, _g, column in applied(X, h, 1, count_r, c, 0, gnd_r):
                R[h, k, pl.ds(c, TILE), :] = jnp.where(column == src_r[k], 1.0, 0.0) - a
            return 0

        def pass_w(t, _):
            c = pl.multiple_of(t * TILE, TILE)
            for k, a, _mid, _g, _column in applied(R, h, 0, count_w, c, 1, gnd_w):
                W[h, k, pl.ds(c, TILE), :] = a
            return 0

        def pass_u(t, acc):
            c = pl.multiple_of(t * TILE, TILE)
            at = pl.ds(c, TILE)
            to = pl.ds(c - PAD, TILE)
            for k, u, w, grounded, column in applied(W, h, 0, rows, c, 2, gnd_u):
                r = R[h, 2 + k, at, :]
                x = X[h, rows + k, at, :]
                if h < halves - 1:
                    U[h, k, to, :] = u
                else:
                    for place, value in enumerate((x, r, w, u)):
                        field_ref[place, k, to, :] = value
                terms = (r * r, r * w, w * w, w * u)
                sourced = column == src_u[k]
                acc = tuple(s + term for s, term in zip(acc, terms)) + tuple(
                    jnp.where(sourced, value, s) for s, value in zip(acc[4:7], (x, r, w))) + tuple(
                    jnp.where(grounded, value, s) for s, value in zip(acc[7:], (x, r, w)))
            return acc

        def sweep(lag, step, carry):
            bounds = own_at[h]
            begin, end = (1, tiles - 1) if lag < 3 else (2, tiles - 2)
            offset = PAD // TILE - lag
            final = j == len(bounds) - 2
            start = begin if j == 0 else offset + core + bounds[j]
            count = (end - 1 if final else offset + bounds[j + 1]) - (begin if j == 0 else offset + bounds[j])
            extra = core if j == 0 else 1 - core if final else None
            pairs = count // 2

            def pair(i, carry):
                return step(start + 2 * i + 1, step(start + 2 * i, carry))

            carry = lax.fori_loop(0, pairs, pair, carry)
            if count % 2:
                carry = step(start + 2 * pairs, carry)
            if extra is not None and not (j == 0 and final):
                carry = lax.fori_loop(start + count, start + count + extra, step, carry)
            return carry

        sweep(1, pass_r, 0)
        sweep(2, pass_w, 0)
        return sweep(3, pass_u, acc)

    def sum_copy(h, d):
        return remote(S.at[h, me], S.at[h, me], sum_send.at[0], sum_recv.at[h], (me + d) % n)

    def send_sums(h, acc):
        ends = tuple(at_source - at_ground for at_source, at_ground in zip(acc[4:7], acc[7:]))
        sums = [jnp.sum(s, axis=0, keepdims=True) for s in acc[:4] + ends]
        S[h, me] = jnp.concatenate(sums + [jnp.zeros((1, LANES), jnp.float32)], 0)
        lax.fori_loop(1, n, lambda d, _: (sum_copy(h, d).start(), 0)[1], 0)

    def totals(h):
        arrived(S.at[h, pl.ds(0, n - 1)], sum_recv.at[h])
        total = S[h, 0]
        for k in range(1, n):
            total = total + S[h, k]
        m0, m1, m2, m3, ex, er, ew = (total[k:k + 1] for k in range(7))
        a0 = m0 / m1
        next_norm = a0 * (a0 * m2 - m1)
        ratio = next_norm / m0
        curve = m1 - a0 * (2.0 * m2 - a0 * m3)
        a1 = next_norm / (curve - ratio * next_norm / a0)
        p = a0 + a1 * (1.0 + ratio)
        q = a1 * a0
        drop_ref[h:h + 1, :] = ex + p * er - q * ew
        return p, q

    def finish(h):
        p, q = totals(h)
        p1 = jnp.broadcast_to(p, (TILE, LANES))
        q1 = jnp.broadcast_to(q, (TILE, LANES))

        def last(t, _):
            c = pl.multiple_of(t * TILE, TILE)
            at = pl.ds(c + PAD, TILE)
            to = pl.ds(c, TILE)
            for k in range(rows):
                r = R[h, 2 + k, at, :]
                w = W[h, 1 + k, at, :]
                pot_ref[h, k, to, :] = X[h, rows + k, at, :] + p1 * r - q1 * w
                res_ref[h, k, to, :] = r - p1 * w + q1 * U[h, k, to, :]
            return 0

        lax.fori_loop(0, cols // TILE, last, 0)

    for h in range(halves):
        side_wait(h)
        cross_wait(h, 0)

        @pl.when(has_diagonal)
        def _():
            cross_wait(h, 1)

    sums = [zeros() for _ in range(halves)]
    relayed = [0] * halves

    def advance(h, k):
        while relayed[h] < parts[h] and pass_at[h][relayed[h]] < own_at[h][k + 1]:
            j = relayed[h]

            @pl.when(gets_relay)
            def _():
                arrived(X.at[h, far_rows, span(pass_at[h], j), :], relay_recv.at[pass_sem[h] + j])
            relayed[h] += 1

        arrived(X.at[h, (1 - odd) * 2 * rows + odd * (rows - 1), span(own_at[h], k), :],
                near_recv.at[own_sem[h] + k])
        sums[h] = compute(h, k, sums[h])

    for k in range(early):
        advance(0, k)
    for h in range(1, halves):
        for j in range(parts[h]):
            relay(h, j)
            onward(h, j)
    for h in range(halves):
        for k in range(0 if h else early, len(own_weights[h])):
            advance(h, k)
        send_sums(h, sums[h])

    for h in range(halves - 1):
        finish(h)

    p, q = totals(halves - 1)
    coef_ref[...] = jnp.concatenate([p, q, jnp.zeros((TILE - 2, LANES), jnp.float32)], 0)

    drained(C.at[0], cond_send.at[0])

    @pl.when(has_above)
    def _():
        drained(C.at[0, pl.ds(0, rows), :], cond_send.at[1])
        drained(C.at[0, :, pl.ds(0, LANES)], cond_send.at[3])

    @pl.when(has_below)
    def _():
        drained(C.at[0, pl.ds(0, rows), :], cond_send.at[2])
        drained(C.at[0, :, pl.ds(0, LANES)], cond_send.at[4])

    drained(X.at[:, pl.ds(0, rows), pl.ds(0, TILE), :], side_send.at[0])
    drained(X.at[:, pl.ds(0, rows - 1), pl.ds(0, TILE), :], cross_send.at[0])
    drained(X.at[:, pl.ds(0, rows - 1), pl.ds(0, TILE), :], edge_send.at[0])
    drained(X.at[:, pl.ds(0, 1), pl.ds(0, cols - TILE), :], near_send.at[0])
    drained(X.at[:, pl.ds(0, rows - 2), pl.ds(0, cols - TILE), :], pass_send.at[0])

    @pl.when(has_diagonal)
    def _():
        drained(X.at[:, pl.ds(0, rows - 1), pl.ds(0, TILE), :], cross_send.at[1])
        drained(X.at[:, pl.ds(0, rows - 1), pl.ds(0, TILE), :], far_send.at[0])

    @pl.when(can_relay)
    def _():
        drained(X.at[:, pl.ds(0, rows - 2), pl.ds(0, cols - TILE), :], relay_send.at[0])

    @pl.when(gets_relay)
    def _():
        drained(X.at[:, pl.ds(0, 1), pl.ds(0, cols - TILE), :], third_send.at[0])

    for h, j in lends:
        @pl.when(can_relay & jnp.logical_not(detours(pairs - 1 - rank, h, j)))
        def _():
            drained(X.at[h, guest, span(pass_at[h], j), :], onward_send.at[pass_sem[h] + j])

        if can_detour(h, j):
            @pl.when(can_relay & detours(rank + 1, h, j))
            def _():
                drained(X.at[h, lent, span(pass_at[h], j), :], forward_send.at[pass_sem[h] + j])

    drained(S.at[:, pl.ds(0, n - 1)], sum_send.at[0])


def closing(pot_ref, res_ref, field_ref, coef_ref, drop_ref, pot_out, res_out, drop_out,
            P1, Q1, sem):
    rows, cols = field_ref.shape[1], field_ref.shape[2]
    before = pot_ref.shape[0]

    def put(ref, out, h, c, count, k):
        return pltpu.make_async_copy(
            ref.at[:, pl.ds(c, count), :],
            out.at[0, :, pl.ds(c, count), pl.ds(h * LANES, LANES)], sem.at[k])

    for h in range(before):
        put(pot_ref.at[h], pot_out, h, 0, cols, 0).start()
        put(res_ref.at[h], res_out, h, 0, cols, 1).start()
    drop = pltpu.make_async_copy(drop_ref, drop_out, sem.at[2])
    drop.start()

    p1 = jnp.broadcast_to(coef_ref[0:1, :], (TILE, LANES))
    q1 = jnp.broadcast_to(coef_ref[1:2, :], (TILE, LANES))
    pieces = 4
    step = cols // pieces

    def last(t, _):
        c = pl.multiple_of(t * TILE, TILE)
        at = pl.ds(c, TILE)
        for k in range(rows):
            x, r, w, u = (field_ref[place, k, at, :] for place in range(4))
            P1[k, at, :] = x + p1 * r - q1 * w
            Q1[k, at, :] = r - p1 * w + q1 * u
        return 0

    for piece in range(pieces):
        lax.fori_loop(piece * step // TILE, (piece + 1) * step // TILE, last, 0, unroll=2)
        put(P1, pot_out, before, piece * step, step, 0).start()
        put(Q1, res_out, before, piece * step, step, 1).start()

    for k, out in enumerate((pot_out, res_out)):
        pltpu.make_async_copy(out, out, sem.at[k]).wait()
    drop.wait()


def solution(mesh):
    n = mesh.shape["tile"]
    rounds = max(1, (n // 2 - 1).bit_length())

    def shards(habitat, table, source_cell, ground_cell, start_potential):
        _, rows, cols, rhs = start_potential.shape
        halves = rhs // LANES
        width = cols + 2 * PAD
        f32 = jnp.float32
        dma = pltpu.SemaphoreType.DMA
        field = jax.ShapeDtypeStruct(start_potential.shape, f32)
        part = jax.ShapeDtypeStruct((halves - 1, rows, cols, LANES), f32)
        drops = jax.ShapeDtypeStruct((halves, LANES), f32)
        vmem = pl.BlockSpec(memory_space=pltpu.VMEM)
        hbm = pl.BlockSpec(memory_space=pltpu.HBM)
        pass_weights = ((32, 31),) * (halves - 1) + ((14, 14, 14, 12, 9),)
        own_weights = ((32, 20, 11),) * (halves - 1) + ((11, 11, 11, 11, 8, 7, 4),)
        passes, owns = sum(map(len, pass_weights)), sum(map(len, own_weights))
        stages = pl.pallas_call(
            functools.partial(kernel, n, rows, cols, rounds, pass_weights, own_weights),
            out_shape=(part, part, jax.ShapeDtypeStruct((4, rows, cols, LANES), f32),
                       jax.ShapeDtypeStruct((TILE, LANES), f32), drops),
            in_specs=[hbm] * 5,
            out_specs=(vmem,) * 5,
            scratch_shapes=[
                pltpu.VMEM((halves, 3 * rows, width, LANES), f32),
                pltpu.VMEM((halves, 2 * rows, width, LANES), f32),
                pltpu.VMEM((halves, 2 * rows - 2, width, LANES), f32),
                pltpu.VMEM((halves - 1, rows, cols, LANES), f32),
                pltpu.VMEM((2 * rows + 1, width, LANES), f32),
                pltpu.VMEM((2 * rows, width, LANES), f32),
                pltpu.VMEM((2 * rows, width, LANES), f32),
                pltpu.VMEM((6, 2 * rows, cols), f32),
                pltpu.VMEM((width, LANES), f32),
                pltpu.VMEM((width, LANES), f32),
                pltpu.VMEM((width, LANES), f32),
                pltpu.VMEM((halves, n, TILE, LANES), f32),
                pltpu.SMEM(table.shape, f32),
                pltpu.VMEM(habitat.shape, jnp.int32),
                pltpu.VMEM((halves, LANES), jnp.int32),
                pltpu.VMEM((halves, LANES), jnp.int32),
                dma((4,)), dma((halves,)),
                dma((5,)), dma((halves,)), dma((halves, 2)), dma((halves, 2)),
                dma((passes,)), dma((passes,)), dma((passes,)), dma((passes,)), dma((owns,)),
                dma((halves,)), dma((5,)), dma((1,)), dma((2,)),
                dma((1,)), dma((1,)), dma((1,)), dma((1,)), dma((1,)), dma((1,)),
                dma((passes,)), dma((passes,)), dma((1,)),
                pltpu.SemaphoreType.REGULAR((rounds,)),
            ],
            compiler_params=pltpu.CompilerParams(
                collective_id=0, has_side_effects=True, vmem_limit_bytes=32 * 2**20),
        )(*(pltpu.with_memory_space_constraint(value, pltpu.HBM) for value in (
            table, habitat, source_cell.reshape(halves, LANES),
            ground_cell.reshape(halves, LANES), start_potential)))
        potentials, residual, drop = pl.pallas_call(
            closing,
            out_shape=(field, field, drops),
            in_specs=[vmem] * 5,
            out_specs=(hbm,) * 3,
            scratch_shapes=[
                pltpu.VMEM((rows, cols, LANES), f32),
                pltpu.VMEM((rows, cols, LANES), f32),
                dma((3,)),
            ],
            compiler_params=pltpu.CompilerParams(vmem_limit_bytes=16 * 2**20),
        )(*stages)
        return potentials, residual, drop.reshape(rhs)

    placed = (
        P(("grp", "tile"), None, None),
        P(),
        P("grp"),
        P("grp"),
        P(("grp", "tile"), None, None, None),
    )
    return jax.shard_map(
        shards,
        mesh=mesh,
        in_specs=placed,
        out_specs=(placed[4], placed[4], P("grp")),
        check_vma=False,
    )
```
